32 devices in a mesh: groups: 2 (over y), section: 4 (over z), tp: 2 (over core), sp: 2 (over x).
Axes of the slice: x: 2, y: 2, z: 4, core: 2. Of those that a mesh axis runs over, the one named last changes fastest.
Arguments:
- hidden: bfloat16 [1024, 6144], P(('groups', 'sp', 'section'), 'tp'), parts along dimension 0, may hold values from -6 to 6
- modulation: float32 [2, 6144], P(None, 'tp'), may hold values from -2 to 2
- time_embed: float32 [12288], P(('groups', 'tp')), parts along dimension 0, may hold values from -2 to 2
- head_weight: bfloat16 [6144, 64], P('tp'), may hold values from -0.078125 to 0.078125
- head_bias: float32 [64], replicated, may hold values from -2 to 2
- noisy: bfloat16 [16, 16, 16, 16], P(('groups', 'sp'), None, 'section'), parts along dimension 0, may hold values from -6 to 6
- step_size: float32 [2], P('groups'), parts along dimension 0, may hold values from 0.2 to 0.6
- latent_mean: float32 [16], replicated, may hold values from -2 to 2
- latent_std: float32 [16], replicated, may hold values from 0.5 to 2
- in_weight: bfloat16 [27, 16, 512], P(None, None, 'tp'), may hold values from -0.3125 to 0.3125
- in_bias: float32 [512], P('tp'), may hold values from -2 to 2
- norm_gain: float32 [512], replicated, may hold values from 0.25 to 1.75
- conv_weight: bfloat16 [27, 512, 512], P(None, 'section', 'tp'), may hold values from -0.0546875 to 0.0546875
- conv_bias: float32 [512], P('tp'), may hold values from -2 to 2
Outputs:
- decoded: bfloat16 [16, 16, 16, 512], P(('groups', 'sp'), None, 'section', 'tp'), parts along dimension 0
The draws below stay inside these ranges and needn't reach their ends.
There are 2 independent parts, one for each index of `groups`. The reference program is written for one: setup_inputs(seed, part) draws one part's arguments, and reference() takes and returns one part's arrays. A program takes and returns all parts, laid end to end along the dimension named above; an argument that names none is the same for every part. Nothing has to cross between parts.
All inputs are finite; a program needn't handle non-finite values.
Results may differ from the reference program's by a relative error of at most 0.006.
Values may be sent and summed in bfloat16 or wider, within the bound.
A program may use at most 128 MiB of HBM per device.

```python
import math
import jax
import jax.numpy as jnp
from jax import lax

D = 6144
LAT_CH = 16
CH = 512
HEIGHT = 16
PCH = 64
FRAMES = 8
WIDTH = 16
TOKENS = 512


def block_scale(own_key, dims, shards, low, high):
    gain = 1.0
    for dim, blocks in shards:
        steps = jax.random.uniform(jax.random.fold_in(jax.random.fold_in(own_key, 6), dim), (blocks,), jnp.float32, low / len(shards), high / len(shards))
        gain = gain * jnp.repeat(jnp.exp(steps), dims[dim] // blocks).reshape((-1,) + (1,) * (len(dims) - 1 - dim))
    return gain


def gaussian(stream_key, dims, scale, bound, cuts=(), dtype=jnp.bfloat16):
    values = scale * jax.random.normal(stream_key, dims, jnp.float32)
    if cuts:
        values = values * block_scale(stream_key, dims, cuts, -0.22, 0.18)
    return jnp.clip(values, -bound, bound).astype(dtype)


def setup_inputs(seed: int = 0, part: int = 0) -> dict:
    arg_keys = jax.random.split(jax.random.key(seed), 15)
    part_splits = jax.random.split(jax.random.fold_in(arg_keys[14], part), 15)
    return {
        "hidden": gaussian(part_splits[0], (TOKENS, D), 1.0, 6.0, ((0, 8), (1, 2))),
        "modulation": gaussian(arg_keys[1], (2, D), 0.3, 2.0, ((1, 2),), jnp.float32),
        "time_embed": gaussian(part_splits[2], (D,), 0.3, 2.0, ((0, 2),), jnp.float32),
        "head_weight": gaussian(arg_keys[3], (D, PCH), D ** -0.5, 0.078125, ((0, 2),)),
        "head_bias": gaussian(arg_keys[4], (PCH,), 0.3, 2.0, (), jnp.float32),
        "noisy": gaussian(part_splits[5], (FRAMES, HEIGHT, WIDTH, LAT_CH), 1.0, 6.0, ((0, 2), (2, 4))),
        "step_size": jnp.clip(jax.random.uniform(part_splits[6], (1,), jnp.float32, 0.2, 0.6), 0.2, 0.6),
        "latent_mean": gaussian(arg_keys[7], (LAT_CH,), 0.5, 2.0, (), jnp.float32),
        "latent_std": jnp.clip(jnp.exp(jax.random.uniform(arg_keys[8], (LAT_CH,), jnp.float32, math.log(0.5), math.log(2.0))), 0.5, 2.0),
        "in_weight": gaussian(arg_keys[9], (27, LAT_CH, CH), (27 * LAT_CH) ** -0.5, 0.3125, ((2, 2),)),
        "in_bias": gaussian(arg_keys[10], (CH,), 0.3, 2.0, ((0, 2),), jnp.float32),
        "norm_gain": jnp.clip(1.0 + 0.15 * jax.random.normal(arg_keys[11], (CH,), jnp.float32), 0.25, 1.75),
        "conv_weight": gaussian(arg_keys[12], (27, CH, CH), (27 * CH) ** -0.5, 0.0546875, ((1, 4), (2, 2))),
        "conv_bias": gaussian(arg_keys[13], (CH,), 0.3, 2.0, ((0, 2),), jnp.float32),
    }


def conv_taps(padded, weight, frames, height, columns):
    channels = padded.shape[3]
    result = jnp.zeros((frames * height * columns, weight.shape[2]), jnp.float32)
    for offset_time in range(3):
        for offset_row in range(3):
            for offset_col in range(3):
                window = padded[offset_time:offset_time + frames, offset_row:offset_row + height, offset_col:offset_col + columns]
                result = result + jnp.dot(window.reshape(-1, channels), weight[9 * offset_time + 3 * offset_row + offset_col], preferred_element_type=jnp.float32)
    return result

def activate(source, gain_vector):
    values = source.astype(jnp.float32)
    squares = lax.optimization_barrier(jnp.mean(values * values, axis=-1, keepdims=True))
    return jax.nn.silu(values * lax.rsqrt(squares + 1e-06) * gain_vector).astype(jnp.bfloat16)

def reference(hidden, modulation, time_embed, head_weight, head_bias, noisy, step_size, latent_mean, latent_std, in_weight, in_bias, norm_gain, conv_weight, conv_bias):
    values = hidden.astype(jnp.float32)
    average = lax.optimization_barrier(jnp.sum(values, axis=1)) / D
    variance = lax.optimization_barrier(jnp.sum(values * values, axis=1)) / D - average * average
    shift_term = modulation[0] + time_embed
    scale_term = modulation[1] + time_embed
    modulated = ((values - average[:, None]) * lax.rsqrt(variance[:, None] + 1e-06) * (1.0 + scale_term) + shift_term).astype(jnp.bfloat16)
    velocity = (jnp.dot(modulated, head_weight, preferred_element_type=jnp.float32) + head_bias).astype(jnp.bfloat16)
    latent_field = velocity.reshape(FRAMES, HEIGHT // 2, WIDTH // 2, 2, 2, LAT_CH)
    latent_field = jnp.transpose(latent_field, (0, 1, 3, 2, 4, 5)).reshape(FRAMES, HEIGHT, WIDTH, LAT_CH)
    latent = ((noisy.astype(jnp.float32) - step_size[0] * latent_field.astype(jnp.float32)) * latent_std + latent_mean).astype(jnp.bfloat16)
    padded = jnp.pad(latent, ((2, 0), (1, 1), (1, 1), (0, 0)))
    upblock = (conv_taps(padded, in_weight, FRAMES, HEIGHT, WIDTH) + in_bias).astype(jnp.bfloat16)
    normed = activate(upblock, norm_gain).reshape(FRAMES, HEIGHT, WIDTH, CH)
    conv_input = jnp.pad(normed, ((2, 0), (1, 1), (1, 1), (0, 0)))
    mixed = conv_taps(conv_input, conv_weight, FRAMES, HEIGHT, WIDTH)
    decoded = (upblock.astype(jnp.float32) + mixed + conv_bias).astype(jnp.bfloat16)
    return decoded.reshape(FRAMES, HEIGHT, WIDTH, CH)
```

```python
import functools

import jax
import jax.numpy as jnp
from jax import lax
from jax.experimental import pallas as pl
from jax.experimental.pallas import tpu as pltpu
from jax.sharding import PartitionSpec as P

D = 6144


def padded_2(value, sides, width):
    for axis, dim in sides:
        count, length = (lax.axis_size(axis), value.shape[dim])
        up = [(i, (i + 1) % count) for i in range(count - 1)]
        down = [(j, i) for i, j in up]
        last = lax.slice_in_dim(value, length - width, length, axis=dim)
        leading = lax.slice_in_dim(value, 0, width, axis=dim)
        before = lax.ppermute(last, axis, up)
        after = lax.ppermute(leading, axis, down)
        value = jnp.concatenate([before, value, after], axis=dim)
    return value


def passed_along(value, axis, by):
    count = lax.axis_size(axis)
    pairs = [(i, i + by) for i in range(count) if 0 <= i + by < count]
    return lax.ppermute(value, axis, pairs)


def conv_taps(padded, weight, frames, height, columns):
    channels = padded.shape[3]
    result = jnp.zeros((frames * height * columns, weight.shape[2]), jnp.float32)
    for offset_time in range(3):
        for offset_row in range(3):
            slab = padded[offset_time : offset_time + frames, offset_row : offset_row + height]
            window = jnp.concatenate(
                [slab[:, :, 0:columns], slab[:, :, 1 : columns + 1], slab[:, :, 2 : columns + 2]],
                axis=3,
            )
            first = 9 * offset_time + 3 * offset_row
            taps = weight[first : first + 3].reshape(3 * channels, weight.shape[2])
            result = result + jnp.dot(
                window.reshape(-1, 3 * channels), taps, preferred_element_type=jnp.float32
            )
    return result


def activate(source, gain_vector):
    values = source.astype(jnp.float32)
    squares = jnp.mean(values * values, axis=-1, keepdims=True)
    return jax.nn.silu(values * lax.rsqrt(squares + 1e-06) * gain_vector).astype(jnp.bfloat16)


def pad_rows(source):
    return jnp.pad(source, ((0, 0), (1, 1), (0, 0), (0, 0)))


def shards(
    hidden,
    modulation,
    time_embed,
    head_weight,
    head_bias,
    noisy,
    step_size,
    latent_mean,
    latent_std,
    in_weight,
    in_bias,
    norm_gain,
    conv_weight,
    conv_bias,
):
    frames, height, columns, lat_channels = noisy.shape
    sections = lax.axis_size("section")
    half_channels = in_weight.shape[2]
    values = hidden.astype(jnp.float32)
    row_sums, square_sums = lax.psum(
        (jnp.sum(values, axis=1), jnp.sum(values * values, axis=1)), "tp"
    )
    average = row_sums / D
    variance = square_sums / D - average * average
    shift_term = modulation[0] + time_embed
    scale_term = modulation[1] + time_embed
    modulated = (
        (values - average[:, None]) * lax.rsqrt(variance[:, None] + 1e-06) * (1.0 + scale_term)
        + shift_term
    ).astype(jnp.bfloat16)
    partial_sum = jnp.dot(modulated, head_weight, preferred_element_type=jnp.float32)
    velocity = (lax.psum(partial_sum, "tp") + head_bias).astype(jnp.bfloat16)
    band_rows = velocity.shape[0] * 2 // (columns * sections)
    outgoing = velocity.reshape(band_rows, sections, -1)
    arrived = lax.all_to_all(outgoing, "section", split_axis=1, concat_axis=0, tiled=True)
    latent_field = arrived.reshape(frames, height // 2, columns // 2, 2, 2, lat_channels)
    latent_field = jnp.transpose(latent_field, (0, 1, 3, 2, 4, 5)).reshape(
        frames, height, columns, lat_channels
    )
    latent = (
        (noisy.astype(jnp.float32) - step_size[0] * latent_field.astype(jnp.float32)) * latent_std
        + latent_mean
    ).astype(jnp.bfloat16)
    latent_wide = padded_2(latent, (("section", 2),), 2)
    earlier = passed_along(latent_wide, "sp", 1)
    stacked = pad_rows(jnp.concatenate([earlier, latent_wide], axis=0))
    extended = (conv_taps(stacked, in_weight, frames + 2, height, columns + 2) + in_bias).astype(
        jnp.bfloat16
    )
    extended = extended.reshape(frames + 2, height, columns + 2, half_channels)
    upblock_half = extended[2:, :, 1 : columns + 1]
    extended_full = lax.all_gather(extended, "tp", axis=3, tiled=True)
    normed = activate(extended_full, norm_gain)
    frame_index = lax.axis_index("sp") * frames - 2 + jnp.arange(frames + 2, dtype=jnp.int32)
    column_index = (
        lax.axis_index("section") * columns - 1 + jnp.arange(columns + 2, dtype=jnp.int32)
    )
    inside_cols = (column_index >= 0) & (column_index < columns * sections)
    inside = (frame_index >= 0)[:, None, None, None] & inside_cols[None, None, :, None]
    conv_input = pad_rows(jnp.where(inside, normed, jnp.zeros_like(normed)))
    full_weight = lax.all_gather(conv_weight, "section", axis=1, tiled=True)
    mixed = conv_taps(conv_input, full_weight, frames, height, columns)
    decoded = (
        upblock_half.astype(jnp.float32).reshape(-1, half_channels) + mixed + conv_bias
    ).astype(jnp.bfloat16)
    return decoded.reshape(frames, height, columns, half_channels)


def iota(shape, dim):
    return lax.broadcasted_iota(jnp.int32, shape, dim)


def dot(left, right):
    return jnp.dot(left, right, preferred_element_type=jnp.float32)


def pieces(value):
    high = value.astype(jnp.bfloat16)
    rest = value - high.astype(jnp.float32)
    middle = rest.astype(jnp.bfloat16)
    low = (rest - middle.astype(jnp.float32)).astype(jnp.bfloat16)
    return high.astype(jnp.float32), middle.astype(jnp.float32), low.astype(jnp.float32)


def block_kernel(
    sizes,
    hidden,
    terms,
    head_weight,
    head_bias,
    noisy,
    step_size,
    latent_affine,
    in_weight,
    in_bias,
    norm_gain,
    conv_bias,
    conv_weight,
    out,
    part_a,
    part_s,
    part_w,
    peer_a,
    peer_s,
    peer_w,
    peer_weight,
    peer_bias,
    fields,
    noises,
    expanded,
    stacked,
    taps_in,
    ups,
    wide,
    weight,
    send_buf,
    recv_buf,
    weight_sem,
    pair_send,
    pair_recv,
    noise_send,
    noise_recv,
    field_send,
    field_recv,
    sum_send,
    sum_recv,
):
    sections, clips_sp, frames, height, columns, lat, channels = sizes
    rows_i, cols_j = height // 2, columns * sections // 2
    width = columns * sections
    tokens = rows_i * cols_j
    near = frames + 2
    half = in_weight.shape[2]
    sec, core, spi = lax.axis_index("section"), lax.axis_index("tp"), lax.axis_index("sp")
    nxt, prv = lax.rem(spi + 1, clips_sp), lax.rem(spi + clips_sp - 1, clips_sp)
    peer = {"tp": 1 - core}

    load = pltpu.make_async_copy(conv_weight, weight, weight_sem)
    load.start()
    barrier = pltpu.get_barrier_semaphore()
    pl.semaphore_signal(barrier, inc=1, device_id=peer)
    for k in range(1, sections):
        pl.semaphore_signal(barrier, inc=1, device_id={"section": lax.rem(sec + k, sections)})
    for k in range(sections):
        pl.semaphore_signal(
            barrier, inc=1, device_id={"section": lax.rem(sec + k, sections), "sp": prv}
        )
    pl.semaphore_wait(barrier, 2 * sections)

    def pair_copy(n, source, target):
        return pltpu.make_async_remote_copy(
            source, target, pair_send.at[n], pair_recv.at[n], device_id=peer
        )

    def spread(source, target, send, recv):
        made = []
        for k in range(1, sections):
            made.append(
                pltpu.make_async_remote_copy(
                    source, target.at[0, k], send.at[0, k], recv.at[0, k],
                    device_id={"section": lax.rem(sec + k, sections)},
                )
            )
        for k in range(sections):
            made.append(
                pltpu.make_async_remote_copy(
                    source, target.at[1, k], send.at[1, k], recv.at[1, k],
                    device_id={"section": lax.rem(sec + k, sections), "sp": nxt},
                )
            )
        return made

    early = [pair_copy(0, in_weight, peer_weight), pair_copy(1, in_bias, peer_bias)]
    noise_copies = spread(noisy, noises, noise_send, noise_recv)
    for c in early + noise_copies:
        c.start()

    features = hidden.shape[1]
    values = hidden[...].astype(jnp.float32)
    own_sum = jnp.sum(values, axis=1, keepdims=True)
    own_square = jnp.sum(values * values, axis=1, keepdims=True)
    center = own_sum / features
    scale, shift = terms[0:1, :], terms[1:2, :]
    centred = ((values - center) * scale).astype(jnp.bfloat16)
    part_a[...] = dot(centred, head_weight[...])
    part_s[...] = jnp.where(iota(part_s.shape, 1) < part_s.shape[1] // 2, own_sum, own_square)
    row = iota((8, features), 0)
    lines = jnp.zeros((8, features), jnp.float32)
    for n, piece in enumerate(pieces(scale) + pieces(shift)):
        lines = jnp.where(row == n, piece, lines)
    made = dot(lines.astype(jnp.bfloat16), head_weight[...])
    line = iota(made.shape, 0)
    own_scale = jnp.sum(jnp.where(line < 3, made, 0.0), axis=0, keepdims=True)
    own_shift = jnp.sum(jnp.where(line >= 3, made, 0.0), axis=0, keepdims=True)
    part_w[...] = jnp.where(line == 0, own_scale, own_shift)
    pair = [
        pair_copy(2, part_a, peer_a), pair_copy(3, part_s, peer_s), pair_copy(4, part_w, peer_w)
    ]
    for c in pair:
        c.start()
    for c in pair:
        c.wait()
    far_sum = peer_s[:, 0:1]
    far_square = peer_s[:, part_s.shape[1] // 2 : part_s.shape[1] // 2 + 1]
    average = (own_sum + far_sum) / D
    variance = (own_square + far_square) / D - average * average
    body = (
        part_a[...]
        + peer_a[...]
        - (average - center) * own_scale
        - (average - far_sum / features) * peer_w[0:1, :]
    )
    velocity = (
        lax.rsqrt(variance + 1e-06) * body + (own_shift + peer_w[1:2, :]) + head_bias[...]
    ).astype(jnp.bfloat16)
    to, at = iota((tokens, tokens), 0), iota((tokens, tokens), 1)
    swap = (lax.rem(to, rows_i) * cols_j + lax.div(to, rows_i) == at).astype(jnp.bfloat16)
    fields[0, 0] = dot(swap, velocity).astype(jnp.bfloat16)
    noises[0, 0] = noisy[...]
    field_copies = spread(fields.at[0, 0], fields, field_send, field_recv)
    for c in field_copies:
        c.start()

    for c in early:
        c.wait()
    taps_in[...] = jnp.zeros_like(taps_in)
    line_size = 4 * 2 * lat
    for q in range(2):
        for e in range(3):
            col = q + e
            step_j, odd = (col + 1) // 2 - q, (col + 1) % 2
            for a in range(3):
                for b in range(3):
                    tap = 9 * a + 3 * b + e
                    for p in range(2):
                        first = step_j * 3 * line_size + a * line_size + (p + b) * 2 * lat + odd * lat
                        left = p * 2 * half
                        taps_in[q, first : first + lat, left : left + half] = in_weight[tap]
                        taps_in[q, first : first + lat, left + half : left + 2 * half] = peer_weight[tap]
    expanded[...] = jnp.zeros_like(expanded)
    wide[0] = jnp.zeros_like(wide[0])
    wide[width + 1] = jnp.zeros_like(wide[0])
    for c in noise_copies + field_copies:
        c.wait()

    lanes = 4 * lat
    src, dst = iota((lanes, line_size), 0), iota((lanes, line_size), 1)
    place_mid = (src + 2 * lat == dst).astype(jnp.bfloat16)
    place_before = ((src == dst + 2 * lat) & (dst < 2 * lat)).astype(jnp.bfloat16)
    place_after = ((src + 6 * lat == dst) & (dst >= 6 * lat)).astype(jnp.bfloat16)
    i_row = lax.rem(iota((tokens, lanes), 0), rows_i)
    step = step_size[0]
    pairs_j = cols_j // sections
    for slot in range(2):
        alive = jnp.float32(1.0) if slot == 0 else (spi > 0).astype(jnp.float32)
        noise_parts = []
        for g in range(sections):
            k = lax.rem(sec + sections - g, sections)
            noise_parts.append(
                noises[slot, k].astype(jnp.float32).reshape(pairs_j, frames, rows_i, lanes)
            )
        for f in range(frames):
            k = lax.rem(sec + sections - f, sections)
            field = fields[slot, k].astype(jnp.float32)
            noise = jnp.concatenate([part[:, f] for part in noise_parts], axis=0)
            noise = noise.reshape(tokens, lanes)
            latent = (noise - step * field) * latent_affine[0:1, :] + latent_affine[1:2, :]
            latent = (latent * alive).astype(jnp.bfloat16).astype(jnp.float32)
            before = jnp.where(i_row == 0, 0.0, pltpu.roll(latent, 1, 0))
            after = jnp.where(i_row == rows_i - 1, 0.0, pltpu.roll(latent, tokens - 1, 0))
            line_values = (
                dot(before.astype(jnp.bfloat16), place_before)
                + dot(latent.astype(jnp.bfloat16), place_mid)
                + dot(after.astype(jnp.bfloat16), place_after)
            )
            expanded[1 : cols_j + 1, f + (1 - slot) * frames] = line_values.reshape(
                cols_j, rows_i, line_size
            )
    block = near * rows_i
    for j in range(cols_j + 2):
        for a in range(3):
            stacked[j * block : (j + 1) * block, a * line_size : (a + 1) * line_size] = (
                expanded[j, a : a + near].reshape(block, line_size).astype(jnp.bfloat16)
            )
    parts = half // channels
    tall = near * height
    for q in range(2):
        lhs = jnp.concatenate(
            [
                stacked[q * block : (q + cols_j) * block, :],
                stacked[(q + 1) * block : (q + 1 + cols_j) * block, :],
            ],
            axis=1,
        )
        for p in range(2):
            for h in range(2):
                left = (p * 2 + h) * half
                bias = in_bias[...] if h == 0 else peer_bias[...]
                up = dot(lhs, taps_in[q, :, left : left + half]) + bias
                up = up.astype(jnp.bfloat16).astype(jnp.float32)
                for j in range(cols_j):
                    for n in range(parts):
                        ups[
                            h * parts + n, pl.ds((2 * j + q) * tall + p, block, stride=2), :
                        ] = up[j * block : (j + 1) * block, n * channels : (n + 1) * channels]

    mine = lax.rem(sec + parts * core, 2 * parts)
    gain = norm_gain[pl.ds(sec, 1), :]
    h_row = lax.rem(iota((tall, channels), 0), height)
    valid = (spi > 0) | (iota((tall, channels), 0) >= 2 * height)

    def normalise(w, carry):
        at_w = pl.ds(pl.multiple_of(w * tall, tall), tall)
        squares = jnp.zeros((tall, channels), jnp.float32)
        for n in range(2 * parts):
            g = ups[n, at_w, :]
            squares = squares + g * g
        mean = jnp.sum(squares, axis=1, keepdims=True) / (2 * half)
        v = ups[mine, at_w, :] * lax.rsqrt(mean + 1e-06) * gain
        v = jnp.where(valid, v / (1.0 + jnp.exp(-v)), 0.0)
        above = jnp.where(h_row == 0, 0.0, pltpu.roll(v, 1, 0))
        below = jnp.where(h_row == height - 1, 0.0, pltpu.roll(v, tall - 1, 0))
        for b, line_v in enumerate((above, v, below)):
            wide[w + 1, :, b * channels : (b + 1) * channels] = line_v.astype(jnp.bfloat16)
        return carry

    lax.fori_loop(0, width, normalise, 0)
    load.wait()

    span = frames * height

    def partial(d):
        total = jnp.zeros((columns * span, weight.shape[2]), jnp.float32)
        for a in range(3):
            for e in range(3):
                window = wide[pl.ds(d * columns + e, columns), a * height : a * height + span, :]
                taps = jnp.concatenate([weight[9 * a + 3 * b + e] for b in range(3)], axis=0)
                total = total + dot(window.reshape(columns * span, 3 * channels), taps)
        return total

    sums = []
    for k in range(1, sections):
        d = lax.rem(sec + k, sections)
        send_buf[k] = partial(d).astype(jnp.bfloat16)
        c = pltpu.make_async_remote_copy(
            send_buf.at[k], recv_buf.at[k], sum_send.at[k], sum_recv.at[k],
            device_id={"section": d},
        )
        c.start()
        sums.append(c)
    total = partial(sec) + conv_bias[...]
    total = total.reshape(columns, span, half)
    own_w = []
    for w in range(columns):
        first = pl.multiple_of((sec * columns + w) * tall + 2 * height, height)
        own_w.append(
            jnp.concatenate([ups[n, pl.ds(first, span), :] for n in range(parts)], axis=1)
        )
    total = total + jnp.stack(own_w)
    for c in sums:
        c.wait()
    for k in range(1, sections):
        total = total + recv_buf[k].astype(jnp.float32).reshape(columns, span, half)
    out[...] = total.astype(out.dtype)


def fused_shards(sizes, *arrays):
    (
        hidden, modulation, time_embed, head_weight, head_bias, noisy, step_size, latent_mean,
        latent_std, in_weight, in_bias, norm_gain, conv_weight, conv_bias,
    ) = arrays
    sections, clips_sp, frames, height, columns, lat, channels = sizes
    rows_i, cols_j, half = height // 2, columns * sections // 2, in_weight.shape[2]
    width, near, tokens, lanes = columns * sections, frames + 2, hidden.shape[0], 4 * lat
    terms = jnp.stack([1.0 + (modulation[1] + time_embed), modulation[0] + time_embed])
    noise = noisy.reshape(frames, rows_i, 2, columns // 2, 2, lat)
    noise = jnp.transpose(noise, (3, 0, 1, 2, 4, 5)).reshape(-1, lanes)
    affine = jnp.stack([jnp.tile(latent_std, 4), jnp.tile(latent_mean, 4)])
    line_size = 8 * lat
    f32, bf16 = jnp.float32, jnp.bfloat16
    vmem, dma = pltpu.VMEM, pltpu.SemaphoreType.DMA
    in_vmem = pl.BlockSpec(memory_space=pltpu.VMEM)
    rows = columns * frames * height
    out = pl.pallas_call(
        functools.partial(block_kernel, sizes),
        out_shape=jax.ShapeDtypeStruct((columns, frames * height, half), bf16),
        in_specs=[in_vmem] * 5
        + [pl.BlockSpec(memory_space=pltpu.SMEM)]
        + [in_vmem] * 5
        + [pl.BlockSpec(memory_space=pl.ANY)],
        out_specs=in_vmem,
        scratch_shapes=[
            vmem((tokens, lanes), f32),
            vmem((tokens, 128), f32),
            vmem((8, lanes), f32),
            vmem((tokens, lanes), f32),
            vmem((tokens, 128), f32),
            vmem((8, lanes), f32),
            vmem(in_weight.shape, bf16),
            vmem((1, half), f32),
            vmem((2, sections, tokens, lanes), bf16),
            vmem((2, sections, tokens, lanes), bf16),
            vmem((cols_j + 2, 2 * frames, rows_i, line_size), f32),
            vmem(((cols_j + 2) * near * rows_i, 3 * line_size), bf16),
            vmem((2, 6 * line_size, 4 * half), bf16),
            vmem((2 * half // channels, width * near * height, channels), f32),
            vmem((width + 2, near * height, 3 * channels), bf16),
            vmem(conv_weight.shape, bf16),
            vmem((sections, rows, half), bf16),
            vmem((sections, rows, half), bf16),
            dma,
            dma((5,)),
            dma((5,)),
            dma((2, sections)),
            dma((2, sections)),
            dma((2, sections)),
            dma((2, sections)),
            dma((sections,)),
            dma((sections,)),
        ],
        compiler_params=pltpu.CompilerParams(collective_id=0, has_side_effects=True),
    )(
        hidden, terms, head_weight, head_bias[None], noise, step_size, affine, in_weight,
        in_bias[None], norm_gain.reshape(-1, channels), conv_bias[None], conv_weight,
    )
    out = out.reshape(columns, frames, height, half)
    return jnp.transpose(out, (1, 2, 0, 3))


def dispatch(*arrays):
    hidden, noisy, in_weight, conv_weight = arrays[0], arrays[5], arrays[9], arrays[12]
    frames, height, columns, lat = noisy.shape
    sections, cores, clips_sp = (lax.axis_size(axis) for axis in ("section", "tp", "sp"))
    channels, half = conv_weight.shape[1:]
    whole_frame = hidden.shape[0] == height // 2 * (columns * sections // 2)
    if (
        whole_frame
        and cores == 2
        and clips_sp > 1
        and frames == sections
        and channels % 128 == 0
        and half % channels == 0
        and lat == 16
        and height == 16
    ):
        sizes = (sections, clips_sp, frames, height, columns, lat, channels)
        return fused_shards(sizes, *arrays)
    return shards(*arrays)


def solution(mesh):
    placed = (
        P(("groups", "sp", "section"), "tp"),
        P(None, "tp"),
        P(("groups", "tp")),
        P("tp", None),
        P(),
        P(("groups", "sp"), None, "section", None),
        P("groups"),
        P(),
        P(),
        P(None, None, "tp"),
        P("tp"),
        P(),
        P(None, "section", "tp"),
        P("tp"),
    )
    return jax.shard_map(
        dispatch,
        mesh=mesh,
        in_specs=placed,
        out_specs=P(("groups", "sp"), None, "section", "tp"),
        check_vma=False,
    )
```

```python
import functools

import jax
import jax.numpy as jnp
from jax import lax
from jax.experimental import pallas as pl
from jax.experimental.pallas import tpu as pltpu
from jax.sharding import PartitionSpec as P

D = 6144


def padded_2(value, sides, width):
    for axis, dim in sides:
        count, length = (lax.axis_size(axis), value.shape[dim])
        up = [(i, (i + 1) % count) for i in range(count - 1)]
        down = [(j, i) for i, j in up]
        last = lax.slice_in_dim(value, length - width, length, axis=dim)
        leading = lax.slice_in_dim(value, 0, width, axis=dim)
        before = lax.ppermute(last, axis, up)
        after = lax.ppermute(leading, axis, down)
        value = jnp.concatenate([before, value, after], axis=dim)
    return value


def passed_along(value, axis, by):
    count = lax.axis_size(axis)
    pairs = [(i, i + by) for i in range(count) if 0 <= i + by < count]
    return lax.ppermute(value, axis, pairs)


def conv_taps(padded, weight, frames, height, columns):
    channels = padded.shape[3]
    result = jnp.zeros((frames * height * columns, weight.shape[2]), jnp.float32)
    for offset_time in range(3):
        for offset_row in range(3):
            slab = padded[offset_time : offset_time + frames, offset_row : offset_row + height]
            window = jnp.concatenate(
                [slab[:, :, 0:columns], slab[:, :, 1 : columns + 1], slab[:, :, 2 : columns + 2]],
                axis=3,
            )
            first = 9 * offset_time + 3 * offset_row
            taps = weight[first : first + 3].reshape(3 * channels, weight.shape[2])
            result = result + jnp.dot(
                window.reshape(-1, 3 * channels), taps, preferred_element_type=jnp.float32
            )
    return result


def activate(source, gain_vector):
    values = source.astype(jnp.float32)
    squares = jnp.mean(values * values, axis=-1, keepdims=True)
    return jax.nn.silu(values * lax.rsqrt(squares + 1e-06) * gain_vector).astype(jnp.bfloat16)


def pad_rows(source):
    return jnp.pad(source, ((0, 0), (1, 1), (0, 0), (0, 0)))


def shards(
    hidden,
    modulation,
    time_embed,
    head_weight,
    head_bias,
    noisy,
    step_size,
    latent_mean,
    latent_std,
    in_weight,
    in_bias,
    norm_gain,
    conv_weight,
    conv_bias,
):
    frames, height, columns, lat_channels = noisy.shape
    sections = lax.axis_size("section")
    half_channels = in_weight.shape[2]
    values = hidden.astype(jnp.float32)
    row_sums, square_sums = lax.psum(
        (jnp.sum(values, axis=1), jnp.sum(values * values, axis=1)), "tp"
    )
    average = row_sums / D
    variance = square_sums / D - average * average
    shift_term = modulation[0] + time_embed
    scale_term = modulation[1] + time_embed
    modulated = (
        (values - average[:, None]) * lax.rsqrt(variance[:, None] + 1e-06) * (1.0 + scale_term)
        + shift_term
    ).astype(jnp.bfloat16)
    partial_sum = jnp.dot(modulated, head_weight, preferred_element_type=jnp.float32)
    velocity = (lax.psum(partial_sum, "tp") + head_bias).astype(jnp.bfloat16)
    band_rows = velocity.shape[0] * 2 // (columns * sections)
    outgoing = velocity.reshape(band_rows, sections, -1)
    arrived = lax.all_to_all(outgoing, "section", split_axis=1, concat_axis=0, tiled=True)
    latent_field = arrived.reshape(frames, height // 2, columns // 2, 2, 2, lat_channels)
    latent_field = jnp.transpose(latent_field, (0, 1, 3, 2, 4, 5)).reshape(
        frames, height, columns, lat_channels
    )
    latent = (
        (noisy.astype(jnp.float32) - step_size[0] * latent_field.astype(jnp.float32)) * latent_std
        + latent_mean
    ).astype(jnp.bfloat16)
    latent_wide = padded_2(latent, (("section", 2),), 2)
    earlier = passed_along(latent_wide, "sp", 1)
    stacked = pad_rows(jnp.concatenate([earlier, latent_wide], axis=0))
    extended = (conv_taps(stacked, in_weight, frames + 2, height, columns + 2) + in_bias).astype(
        jnp.bfloat16
    )
    extended = extended.reshape(frames + 2, height, columns + 2, half_channels)
    upblock_half = extended[2:, :, 1 : columns + 1]
    extended_full = lax.all_gather(extended, "tp", axis=3, tiled=True)
    normed = activate(extended_full, norm_gain)
    frame_index = lax.axis_index("sp") * frames - 2 + jnp.arange(frames + 2, dtype=jnp.int32)
    column_index = (
        lax.axis_index("section") * columns - 1 + jnp.arange(columns + 2, dtype=jnp.int32)
    )
    inside_cols = (column_index >= 0) & (column_index < columns * sections)
    inside = (frame_index >= 0)[:, None, None, None] & inside_cols[None, None, :, None]
    conv_input = pad_rows(jnp.where(inside, normed, jnp.zeros_like(normed)))
    full_weight = lax.all_gather(conv_weight, "section", axis=1, tiled=True)
    mixed = conv_taps(conv_input, full_weight, frames, height, columns)
    decoded = (
        upblock_half.astype(jnp.float32).reshape(-1, half_channels) + mixed + conv_bias
    ).astype(jnp.bfloat16)
    return decoded.reshape(frames, height, columns, half_channels)


def iota(shape, dim):
    return lax.broadcasted_iota(jnp.int32, shape, dim)


def dot(left, right):
    return jnp.dot(left, right, preferred_element_type=jnp.float32)


def dot_rows(left, right):
    return lax.dot_general(
        left, right, (((1,), (1,)), ((), ())), preferred_element_type=jnp.float32
    )


def pieces(value):
    high = value.astype(jnp.bfloat16)
    rest = value - high.astype(jnp.float32)
    middle = rest.astype(jnp.bfloat16)
    low = (rest - middle.astype(jnp.float32)).astype(jnp.bfloat16)
    return high.astype(jnp.float32), middle.astype(jnp.float32), low.astype(jnp.float32)


def block_kernel(
    sizes,
    modulation,
    time_embed,
    head_bias,
    noisy,
    step_size,
    latent_std,
    latent_mean,
    in_bias,
    norm_gain,
    conv_bias,
    hidden_far,
    head_far,
    in_far,
    conv_far,
    out,
    hidden,
    head_weight,
    in_weight,
    part_a,
    part_s,
    part_w,
    peer_a,
    peer_s,
    peer_w,
    peer_weight,
    peer_bias,
    fields,
    noises,
    expanded,
    stacked,
    taps_in,
    ups,
    wide,
    weight,
    send_buf,
    recv_buf,
    final,
    load_sems,
    pair_send,
    pair_recv,
    noise_send,
    noise_recv,
    field_send,
    field_recv,
    sum_send,
    sum_recv,
):
    sections, clips_sp, frames, height, columns, lat, channels = sizes
    rows_i, cols_j = height // 2, columns * sections // 2
    width = columns * sections
    tokens = rows_i * cols_j
    near = frames + 2
    half = in_weight.shape[2]
    sec, core, spi = lax.axis_index("section"), lax.axis_index("tp"), lax.axis_index("sp")
    nxt, prv = lax.rem(spi + 1, clips_sp), lax.rem(spi + clips_sp - 1, clips_sp)
    peer = {"tp": 1 - core}

    loads = [
        pltpu.make_async_copy(source, target, load_sems.at[n])
        for n, (source, target) in enumerate(
            ((hidden_far, hidden), (head_far, head_weight), (in_far, in_weight), (conv_far, weight))
        )
    ]
    for c in loads:
        c.start()
    barrier = pltpu.get_barrier_semaphore()
    pl.semaphore_signal(barrier, inc=1, device_id=peer)
    for k in range(1, sections):
        pl.semaphore_signal(barrier, inc=1, device_id={"section": lax.rem(sec + k, sections)})
    for k in range(sections):
        pl.semaphore_signal(
            barrier, inc=1, device_id={"section": lax.rem(sec + k, sections), "sp": prv}
        )

    def pair_copy(n, source, target):
        return pltpu.make_async_remote_copy(
            source, target, pair_send.at[n], pair_recv.at[n], device_id=peer
        )

    def spread(source, target, send, recv):
        made = []
        for k in range(1, sections):
            made.append(
                pltpu.make_async_remote_copy(
                    source, target.at[0, k], send.at[0, k], recv.at[0, k],
                    device_id={"section": lax.rem(sec + k, sections)},
                )
            )
        for k in range(sections):
            made.append(
                pltpu.make_async_remote_copy(
                    source, target.at[1, k], send.at[1, k], recv.at[1, k],
                    device_id={"section": lax.rem(sec + k, sections), "sp": nxt},
                )
            )
        return made

    lanes = 4 * lat
    share = frames * rows_i * columns // 2
    to, at = iota((4 * share, 4 * share), 0), iota((4 * share, 4 * share), 1)
    cell, token = lax.div(to, share), lax.rem(to, share)
    jl, line_i = lax.div(token, frames * rows_i), lax.rem(token, frames * rows_i)
    home = (2 * line_i + lax.div(cell, 2)) * columns + 2 * jl + lax.rem(cell, 2)
    moved = dot((home == at).astype(jnp.bfloat16), noisy[...]).astype(jnp.bfloat16)
    src, dst = iota((lat, lanes), 0), iota((lat, lanes), 1)
    own_noise = jnp.zeros((share, lanes), jnp.float32)
    for n in range(4):
        own_noise = own_noise + dot(
            moved[n * share : (n + 1) * share], (src + n * lat == dst).astype(jnp.bfloat16)
        )
    noises[0, 0] = own_noise.astype(jnp.bfloat16)

    features = hidden.shape[1]
    scale = 1.0 + (modulation[1:2, :] + time_embed[...])
    shift = modulation[0:1, :] + time_embed[...]
    loads[0].wait()
    values = hidden[...].astype(jnp.float32)
    own_sum = jnp.sum(values, axis=1, keepdims=True)
    own_square = jnp.sum(values * values, axis=1, keepdims=True)
    center = own_sum / features
    centred = ((values - center) * scale).astype(jnp.bfloat16)
    loads[1].wait()
    part_a[...] = dot_rows(centred, head_weight[...])
    part_s[...] = jnp.where(iota(part_s.shape, 1) < part_s.shape[1] // 2, own_sum, own_square)
    row = iota((8, features), 0)
    lines = jnp.zeros((8, features), jnp.float32)
    for n, piece in enumerate(pieces(scale) + pieces(shift)):
        lines = jnp.where(row == n, piece, lines)
    made = dot_rows(lines.astype(jnp.bfloat16), head_weight[...])
    line = iota(made.shape, 0)
    own_scale = jnp.sum(jnp.where(line < 3, made, 0.0), axis=0, keepdims=True)
    own_shift = jnp.sum(jnp.where(line >= 3, made, 0.0), axis=0, keepdims=True)
    part_w[...] = jnp.where(line == 0, own_scale, own_shift)
    pair = [
        pair_copy(2, part_a, peer_a), pair_copy(3, part_s, peer_s), pair_copy(4, part_w, peer_w)
    ]
    loads[2].wait()
    early = [pair_copy(0, in_weight, peer_weight), pair_copy(1, in_bias, peer_bias)]
    noise_copies = spread(noises.at[0, 0], noises, noise_send, noise_recv)
    pl.semaphore_wait(barrier, 2 * sections)
    for c in pair + noise_copies + early:
        c.start()
    for c in pair:
        c.wait()
    far_sum = peer_s[:, 0:1]
    far_square = peer_s[:, part_s.shape[1] // 2 : part_s.shape[1] // 2 + 1]
    average = (own_sum + far_sum) / D
    variance = (own_square + far_square) / D - average * average
    body = (
        part_a[...]
        + peer_a[...]
        - (average - center) * own_scale
        - (average - far_sum / features) * peer_w[0:1, :]
    )
    velocity = (
        lax.rsqrt(variance + 1e-06) * body + (own_shift + peer_w[1:2, :]) + head_bias[...]
    ).astype(jnp.bfloat16)
    to, at = iota((tokens, tokens), 0), iota((tokens, tokens), 1)
    swap = (lax.rem(to, rows_i) * cols_j + lax.div(to, rows_i) == at).astype(jnp.bfloat16)
    fields[0, 0] = dot(swap, velocity).astype(jnp.bfloat16)
    field_copies = spread(fields.at[0, 0], fields, field_send, field_recv)
    for c in field_copies:
        c.start()

    for c in early:
        c.wait()
    taps_in[...] = jnp.zeros_like(taps_in)
    line_size = 4 * 2 * lat
    for q in range(2):
        for e in range(3):
            col = q + e
            step_j, odd = (col + 1) // 2 - q, (col + 1) % 2
            for a in range(3):
                for b in range(3):
                    tap = 9 * a + 3 * b + e
                    for p in range(2):
                        first = step_j * 3 * line_size + a * line_size + (p + b) * 2 * lat + odd * lat
                        left = p * 2 * half
                        taps_in[q, first : first + lat, left : left + half] = in_weight[tap]
                        taps_in[q, first : first + lat, left + half : left + 2 * half] = peer_weight[tap]
    expanded[...] = jnp.zeros_like(expanded)
    wide[0] = jnp.zeros_like(wide[0])
    wide[width + 1] = jnp.zeros_like(wide[0])
    for c in noise_copies + field_copies:
        c.wait()

    src, dst = iota((lanes, line_size), 0), iota((lanes, line_size), 1)
    place_mid = (src + 2 * lat == dst).astype(jnp.bfloat16)
    place_before = ((src == dst + 2 * lat) & (dst < 2 * lat)).astype(jnp.bfloat16)
    place_after = ((src + 6 * lat == dst) & (dst >= 6 * lat)).astype(jnp.bfloat16)
    i_row = lax.rem(iota((tokens, lanes), 0), rows_i)
    step = step_size[0]
    std = jnp.concatenate([latent_std[...]] * 4, axis=1)
    mean_latent = jnp.concatenate([latent_mean[...]] * 4, axis=1)
    pairs_j = cols_j // sections
    for slot in range(2):
        alive = jnp.float32(1.0) if slot == 0 else (spi > 0).astype(jnp.float32)
        noise_parts = []
        for g in range(sections):
            k = lax.rem(sec + sections - g, sections)
            noise_parts.append(
                noises[slot, k].astype(jnp.float32).reshape(pairs_j, frames, rows_i, lanes)
            )
        for f in range(frames):
            k = lax.rem(sec + sections - f, sections)
            field = fields[slot, k].astype(jnp.float32)
            noise = jnp.concatenate([part[:, f] for part in noise_parts], axis=0)
            noise = noise.reshape(tokens, lanes)
            latent = (noise - step * field) * std + mean_latent
            latent = (latent * alive).astype(jnp.bfloat16).astype(jnp.float32)
            before = jnp.where(i_row == 0, 0.0, pltpu.roll(latent, 1, 0))
            after = jnp.where(i_row == rows_i - 1, 0.0, pltpu.roll(latent, tokens - 1, 0))
            line_values = (
                dot(before.astype(jnp.bfloat16), place_before)
                + dot(latent.astype(jnp.bfloat16), place_mid)
                + dot(after.astype(jnp.bfloat16), place_after)
            )
            expanded[1 : cols_j + 1, f + (1 - slot) * frames] = line_values.reshape(
                cols_j, rows_i, line_size
            )
    block = near * rows_i
    for j in range(cols_j + 2):
        for a in range(3):
            stacked[j * block : (j + 1) * block, a * line_size : (a + 1) * line_size] = (
                expanded[j, a : a + near].reshape(block, line_size).astype(jnp.bfloat16)
            )
    parts = half // channels
    tall = near * height
    for q in range(2):
        lhs = jnp.concatenate(
            [
                stacked[q * block : (q + cols_j) * block, :],
                stacked[(q + 1) * block : (q + 1 + cols_j) * block, :],
            ],
            axis=1,
        )
        for p in range(2):
            for h in range(2):
                left = (p * 2 + h) * half
                bias = in_bias[...] if h == 0 else peer_bias[...]
                up = dot(lhs, taps_in[q, :, left : left + half]) + bias
                up = up.astype(jnp.bfloat16).astype(jnp.float32)
                for j in range(cols_j):
                    for n in range(parts):
                        ups[
                            h * parts + n, pl.ds((2 * j + q) * tall + p, block, stride=2), :
                        ] = up[j * block : (j + 1) * block, n * channels : (n + 1) * channels]

    mine = lax.rem(sec + parts * core, 2 * parts)
    gain = norm_gain[pl.ds(sec, 1), :]
    h_row = lax.rem(iota((tall, channels), 0), height)
    valid = (spi > 0) | (iota((tall, channels), 0) >= 2 * height)

    def normalise(w, carry):
        at_w = pl.ds(pl.multiple_of(w * tall, tall), tall)
        squares = jnp.zeros((tall, channels), jnp.float32)
        for n in range(2 * parts):
            g = ups[n, at_w, :]
            squares = squares + g * g
        mean = jnp.sum(squares, axis=1, keepdims=True) / (2 * half)
        v = ups[mine, at_w, :] * lax.rsqrt(mean + 1e-06) * gain
        v = jnp.where(valid, v / (1.0 + jnp.exp(-v)), 0.0)
        above = jnp.where(h_row == 0, 0.0, pltpu.roll(v, 1, 0))
        below = jnp.where(h_row == height - 1, 0.0, pltpu.roll(v, tall - 1, 0))
        for b, line_v in enumerate((above, v, below)):
            wide[w + 1, :, b * channels : (b + 1) * channels] = line_v.astype(jnp.bfloat16)
        return carry

    lax.fori_loop(0, width, normalise, 0)
    loads[3].wait()

    span = frames * height

    def partial(d):
        total = jnp.zeros((columns * span, weight.shape[2]), jnp.float32)
        for a in range(3):
            for e in range(3):
                window = wide[pl.ds(d * columns + e, columns), a * height : a * height + span, :]
                taps = jnp.concatenate([weight[9 * a + 3 * b + e] for b in range(3)], axis=0)
                total = total + dot(window.reshape(columns * span, 3 * channels), taps)
        return total

    sums = []
    for k in [*range(sections // 2, sections), *range(1, sections // 2)]:
        d = lax.rem(sec + k, sections)
        send_buf[k] = partial(d).astype(jnp.bfloat16)
        c = pltpu.make_async_remote_copy(
            send_buf.at[k], recv_buf.at[k], sum_send.at[k], sum_recv.at[k],
            device_id={"section": d},
        )
        c.start()
        sums.append(c)
    total = partial(sec) + conv_bias[...]
    total = total.reshape(columns, span, half)
    own_w = []
    for w in range(columns):
        first = pl.multiple_of((sec * columns + w) * tall + 2 * height, height)
        own_w.append(
            jnp.concatenate([ups[n, pl.ds(first, span), :] for n in range(parts)], axis=1)
        )
    total = total + jnp.stack(own_w)
    for c in sums:
        c.wait()
    for k in range(1, sections):
        total = total + recv_buf[k].astype(jnp.float32).reshape(columns, span, half)
    for w in range(columns):
        for n in range(parts):
            final[n, pl.ds(w, span, stride=columns), :] = total[
                w, :, n * channels : (n + 1) * channels
            ]
    for n in range(parts):
        out[:, n * channels : (n + 1) * channels] = final[n].astype(out.dtype)


def fused_shards(sizes, *arrays):
    (
        hidden, modulation, time_embed, head_weight, head_bias, noisy, step_size, latent_mean,
        latent_std, in_weight, in_bias, norm_gain, conv_weight, conv_bias,
    ) = arrays
    sections, clips_sp, frames, height, columns, lat, channels = sizes
    rows_i, cols_j, half = height // 2, columns * sections // 2, in_weight.shape[2]
    width, near, tokens, lanes = columns * sections, frames + 2, hidden.shape[0], 4 * lat
    line_size = 8 * lat
    f32, bf16 = jnp.float32, jnp.bfloat16
    vmem, dma = pltpu.VMEM, pltpu.SemaphoreType.DMA
    in_vmem = pl.BlockSpec(memory_space=pltpu.VMEM)
    rows = columns * frames * height
    out = pl.pallas_call(
        functools.partial(block_kernel, sizes),
        out_shape=jax.ShapeDtypeStruct((rows, half), bf16),
        in_specs=[in_vmem] * 4
        + [pl.BlockSpec(memory_space=pltpu.SMEM)]
        + [in_vmem] * 5
        + [pl.BlockSpec(memory_space=pl.ANY)] * 4,
        out_specs=in_vmem,
        scratch_shapes=[
            vmem(hidden.shape, bf16),
            vmem(head_weight.shape[::-1], bf16),
            vmem(in_weight.shape, bf16),
            vmem((tokens, lanes), f32),
            vmem((tokens, 128), f32),
            vmem((8, lanes), f32),
            vmem((tokens, lanes), f32),
            vmem((tokens, 128), f32),
            vmem((8, lanes), f32),
            vmem(in_weight.shape, bf16),
            vmem((1, half), f32),
            vmem((2, sections, tokens, lanes), bf16),
            vmem((2, sections, tokens, lanes), bf16),
            vmem((cols_j + 2, 2 * frames, rows_i, line_size), f32),
            vmem(((cols_j + 2) * near * rows_i, 3 * line_size), bf16),
            vmem((2, 6 * line_size, 4 * half), bf16),
            vmem((2 * half // channels, width * near * height, channels), f32),
            vmem((width + 2, near * height, 3 * channels), bf16),
            vmem(conv_weight.shape, bf16),
            vmem((sections, rows, half), bf16),
            vmem((sections, rows, half), bf16),
            vmem((half // channels, rows, channels), f32),
            dma((4,)),
            dma((5,)),
            dma((5,)),
            dma((2, sections)),
            dma((2, sections)),
            dma((2, sections)),
            dma((2, sections)),
            dma((sections,)),
            dma((sections,)),
        ],
        compiler_params=pltpu.CompilerParams(collective_id=0, has_side_effects=True),
    )(
        modulation, time_embed[None], head_bias[None], noisy.reshape(-1, lat), step_size,
        latent_std[None], latent_mean[None], in_bias[None], norm_gain.reshape(-1, channels),
        conv_bias[None], hidden, head_weight.T, in_weight, conv_weight,
    )
    return out.reshape(frames, height, columns, half)


def dispatch(*arrays):
    hidden, noisy, in_weight, conv_weight = arrays[0], arrays[5], arrays[9], arrays[12]
    frames, height, columns, lat = noisy.shape
    sections, cores, clips_sp = (lax.axis_size(axis) for axis in ("section", "tp", "sp"))
    channels, half = conv_weight.shape[1:]
    whole_frame = hidden.shape[0] == height // 2 * (columns * sections // 2)
    if (
        whole_frame
        and cores == 2
        and clips_sp > 1
        and frames == sections
        and channels % 128 == 0
        and half % channels == 0
        and lat == 16
        and height == 16
    ):
        sizes = (sections, clips_sp, frames, height, columns, lat, channels)
        return fused_shards(sizes, *arrays)
    return shards(*arrays)


def solution(mesh):
    placed = (
        P(("groups", "sp", "section"), "tp"),
        P(None, "tp"),
        P(("groups", "tp")),
        P("tp", None),
        P(),
        P(("groups", "sp"), None, "section", None),
        P("groups"),
        P(),
        P(),
        P(None, None, "tp"),
        P("tp"),
        P(),
        P(None, "section", "tp"),
        P("tp"),
    )
    return jax.shard_map(
        dispatch,
        mesh=mesh,
        in_specs=placed,
        out_specs=P(("groups", "sp"), None, "section", "tp"),
        check_vma=False,
    )
```

```python
import functools

import jax
import jax.numpy as jnp
from jax import lax
from jax.experimental import pallas as pl
from jax.experimental.pallas import tpu as pltpu
from jax.sharding import PartitionSpec as P

D = 6144


def padded_2(value, sides, width):
    for axis, dim in sides:
        count, length = (lax.axis_size(axis), value.shape[dim])
        up = [(i, (i + 1) % count) for i in range(count - 1)]
        down = [(j, i) for i, j in up]
        last = lax.slice_in_dim(value, length - width, length, axis=dim)
        leading = lax.slice_in_dim(value, 0, width, axis=dim)
        before = lax.ppermute(last, axis, up)
        after = lax.ppermute(leading, axis, down)
        value = jnp.concatenate([before, value, after], axis=dim)
    return value


def passed_along(value, axis, by):
    count = lax.axis_size(axis)
    pairs = [(i, i + by) for i in range(count) if 0 <= i + by < count]
    return lax.ppermute(value, axis, pairs)


def conv_taps(padded, weight, frames, height, columns):
    channels = padded.shape[3]
    result = jnp.zeros((frames * height * columns, weight.shape[2]), jnp.float32)
    for offset_time in range(3):
        for offset_row in range(3):
            slab = padded[offset_time : offset_time + frames, offset_row : offset_row + height]
            window = jnp.concatenate(
                [slab[:, :, 0:columns], slab[:, :, 1 : columns + 1], slab[:, :, 2 : columns + 2]],
                axis=3,
            )
            first = 9 * offset_time + 3 * offset_row
            taps = weight[first : first + 3].reshape(3 * channels, weight.shape[2])
            result = result + jnp.dot(
                window.reshape(-1, 3 * channels), taps, preferred_element_type=jnp.float32
            )
    return result


def activate(source, gain_vector):
    values = source.astype(jnp.float32)
    squares = jnp.mean(values * values, axis=-1, keepdims=True)
    return jax.nn.silu(values * lax.rsqrt(squares + 1e-06) * gain_vector).astype(jnp.bfloat16)


def pad_rows(source):
    return jnp.pad(source, ((0, 0), (1, 1), (0, 0), (0, 0)))


def shards(
    hidden,
    modulation,
    time_embed,
    head_weight,
    head_bias,
    noisy,
    step_size,
    latent_mean,
    latent_std,
    in_weight,
    in_bias,
    norm_gain,
    conv_weight,
    conv_bias,
):
    frames, height, columns, lat_channels = noisy.shape
    sections = lax.axis_size("section")
    half_channels = in_weight.shape[2]
    values = hidden.astype(jnp.float32)
    row_sums, square_sums = lax.psum(
        (jnp.sum(values, axis=1), jnp.sum(values * values, axis=1)), "tp"
    )
    average = row_sums / D
    variance = square_sums / D - average * average
    shift_term = modulation[0] + time_embed
    scale_term = modulation[1] + time_embed
    modulated = (
        (values - average[:, None]) * lax.rsqrt(variance[:, None] + 1e-06) * (1.0 + scale_term)
        + shift_term
    ).astype(jnp.bfloat16)
    partial_sum = jnp.dot(modulated, head_weight, preferred_element_type=jnp.float32)
    velocity = (lax.psum(partial_sum, "tp") + head_bias).astype(jnp.bfloat16)
    band_rows = velocity.shape[0] * 2 // (columns * sections)
    outgoing = velocity.reshape(band_rows, sections, -1)
    arrived = lax.all_to_all(outgoing, "section", split_axis=1, concat_axis=0, tiled=True)
    latent_field = arrived.reshape(frames, height // 2, columns // 2, 2, 2, lat_channels)
    latent_field = jnp.transpose(latent_field, (0, 1, 3, 2, 4, 5)).reshape(
        frames, height, columns, lat_channels
    )
    latent = (
        (noisy.astype(jnp.float32) - step_size[0] * latent_field.astype(jnp.float32)) * latent_std
        + latent_mean
    ).astype(jnp.bfloat16)
    latent_wide = padded_2(latent, (("section", 2),), 2)
    earlier = passed_along(latent_wide, "sp", 1)
    stacked = pad_rows(jnp.concatenate([earlier, latent_wide], axis=0))
    extended = (conv_taps(stacked, in_weight, frames + 2, height, columns + 2) + in_bias).astype(
        jnp.bfloat16
    )
    extended = extended.reshape(frames + 2, height, columns + 2, half_channels)
    upblock_half = extended[2:, :, 1 : columns + 1]
    extended_full = lax.all_gather(extended, "tp", axis=3, tiled=True)
    normed = activate(extended_full, norm_gain)
    frame_index = lax.axis_index("sp") * frames - 2 + jnp.arange(frames + 2, dtype=jnp.int32)
    column_index = (
        lax.axis_index("section") * columns - 1 + jnp.arange(columns + 2, dtype=jnp.int32)
    )
    inside_cols = (column_index >= 0) & (column_index < columns * sections)
    inside = (frame_index >= 0)[:, None, None, None] & inside_cols[None, None, :, None]
    conv_input = pad_rows(jnp.where(inside, normed, jnp.zeros_like(normed)))
    full_weight = lax.all_gather(conv_weight, "section", axis=1, tiled=True)
    mixed = conv_taps(conv_input, full_weight, frames, height, columns)
    decoded = (
        upblock_half.astype(jnp.float32).reshape(-1, half_channels) + mixed + conv_bias
    ).astype(jnp.bfloat16)
    return decoded.reshape(frames, height, columns, half_channels)


def iota(shape, dim):
    return lax.broadcasted_iota(jnp.int32, shape, dim)


def dot(left, right):
    return jnp.dot(left, right, preferred_element_type=jnp.float32)


def dot_rows(left, right):
    return lax.dot_general(
        left, right, (((1,), (1,)), ((), ())), preferred_element_type=jnp.float32
    )


def passing(source, target, send, recv, section):
    return pltpu.make_async_remote_copy(
        source, target, send, recv, device_id={"section": section}
    )


def pieces(value):
    high = value.astype(jnp.bfloat16)
    rest = value - high.astype(jnp.float32)
    middle = rest.astype(jnp.bfloat16)
    low = (rest - middle.astype(jnp.float32)).astype(jnp.bfloat16)
    return high.astype(jnp.float32), middle.astype(jnp.float32), low.astype(jnp.float32)


def block_kernel(
    sizes,
    modulation,
    time_embed,
    head_bias,
    noisy,
    step_size,
    latent_std,
    latent_mean,
    in_bias,
    norm_gain,
    conv_bias,
    hidden_far,
    head_far,
    in_far,
    conv_far,
    out,
    hidden,
    head_weight,
    in_weight,
    part_a,
    part_s,
    part_w,
    peer_a,
    peer_s,
    peer_w,
    peer_weight,
    peer_bias,
    fields,
    noises,
    noise_own,
    expanded,
    stacked,
    taps_in,
    ups,
    wide,
    weight,
    send_buf,
    recv_buf,
    relay,
    held,
    final,
    load_sems,
    relay_sem,
    pair_send,
    pair_recv,
    noise_send,
    noise_recv,
    field_send,
    field_recv,
    sum_send,
    sum_recv,
):
    sections, clips_sp, frames, height, columns, lat, channels = sizes
    rows_i, cols_j = height // 2, columns * sections // 2
    width = columns * sections
    tokens = rows_i * cols_j
    near = frames + 2
    half = in_weight.shape[2]
    sec, core, spi = lax.axis_index("section"), lax.axis_index("tp"), lax.axis_index("sp")
    nxt, prv = lax.rem(spi + 1, clips_sp), lax.rem(spi + clips_sp - 1, clips_sp)
    peer = {"tp": 1 - core}

    loads = [
        pltpu.make_async_copy(source, target, load_sems.at[n])
        for n, (source, target) in enumerate(
            ((hidden_far, hidden), (head_far, head_weight), (in_far, in_weight), (conv_far, weight))
        )
    ]
    for c in loads:
        c.start()
    barrier = pltpu.get_barrier_semaphore()
    pl.semaphore_signal(barrier, inc=1, device_id=peer)
    for k in range(1, sections):
        pl.semaphore_signal(barrier, inc=1, device_id={"section": lax.rem(sec + k, sections)})
    for k in range(sections):
        pl.semaphore_signal(
            barrier, inc=1, device_id={"section": lax.rem(sec + k, sections), "sp": prv}
        )

    def pair_copy(n, source, target):
        return pltpu.make_async_remote_copy(
            source, target, pair_send.at[n], pair_recv.at[n], device_id=peer
        )

    def spread(source, target, send, recv):
        made = []
        for k in range(1, sections):
            made.append(
                pltpu.make_async_remote_copy(
                    source, target.at[0, k], send.at[0, k], recv.at[0, k],
                    device_id={"section": lax.rem(sec + k, sections)},
                )
            )
        for k in range(sections):
            made.append(
                pltpu.make_async_remote_copy(
                    source, target.at[1, k], send.at[1, k], recv.at[1, k],
                    device_id={"section": lax.rem(sec + k, sections), "sp": nxt},
                )
            )
        return made

    lanes = 4 * lat
    tile = rows_i * columns // 2
    share = frames * tile
    to, at = iota((4 * share, 4 * share), 0), iota((4 * share, 4 * share), 1)
    cell, token = lax.div(to, share), lax.rem(to, share)
    line_f = lax.div(token, tile)
    jl, line_i = lax.div(lax.rem(token, tile), rows_i), line_f * rows_i + lax.rem(token, rows_i)
    home = (2 * line_i + lax.div(cell, 2)) * columns + 2 * jl + lax.rem(cell, 2)
    moved = dot((home == at).astype(jnp.bfloat16), noisy[...]).astype(jnp.bfloat16)
    src, dst = iota((lat, lanes), 0), iota((lat, lanes), 1)
    own_noise = jnp.zeros((share, lanes), jnp.float32)
    for n in range(4):
        own_noise = own_noise + dot(
            moved[n * share : (n + 1) * share], (src + n * lat == dst).astype(jnp.bfloat16)
        )
    noise_own[...] = own_noise.astype(jnp.bfloat16).reshape(noise_own.shape)

    features = hidden.shape[1]
    scale = 1.0 + (modulation[1:2, :] + time_embed[...])
    shift = modulation[0:1, :] + time_embed[...]
    loads[0].wait()
    values = hidden[...].astype(jnp.float32)
    own_sum = jnp.sum(values, axis=1, keepdims=True)
    own_square = jnp.sum(values * values, axis=1, keepdims=True)
    center = own_sum / features
    centred = ((values - center) * scale).astype(jnp.bfloat16)
    loads[1].wait()
    part_a[...] = dot_rows(centred, head_weight[...])
    part_s[...] = jnp.where(iota(part_s.shape, 1) < part_s.shape[1] // 2, own_sum, own_square)
    row = iota((8, features), 0)
    lines = jnp.zeros((8, features), jnp.float32)
    for n, piece in enumerate(pieces(scale) + pieces(shift)):
        lines = jnp.where(row == n, piece, lines)
    made = dot_rows(lines.astype(jnp.bfloat16), head_weight[...])
    line = iota(made.shape, 0)
    own_scale = jnp.sum(jnp.where(line < 3, made, 0.0), axis=0, keepdims=True)
    own_shift = jnp.sum(jnp.where(line >= 3, made, 0.0), axis=0, keepdims=True)
    part_w[...] = jnp.where(line == 0, own_scale, own_shift)
    pair = [
        pair_copy(2, part_a, peer_a), pair_copy(3, part_s, peer_s), pair_copy(4, part_w, peer_w)
    ]
    loads[2].wait()
    early = [pair_copy(0, in_weight, peer_weight), pair_copy(1, in_bias, peer_bias)]
    noise_copies = []
    for k in range(1, sections):
        d = lax.rem(sec + k, sections)
        noise_copies.append(
            pltpu.make_async_remote_copy(
                noise_own.at[d], noises.at[k], noise_send.at[k], noise_recv.at[k],
                device_id={"section": d},
            )
        )
    pl.semaphore_wait(barrier, 2 * sections)
    for c in pair + noise_copies + early:
        c.start()
    for c in pair:
        c.wait()
    far_sum = peer_s[:, 0:1]
    far_square = peer_s[:, part_s.shape[1] // 2 : part_s.shape[1] // 2 + 1]
    average = (own_sum + far_sum) / D
    variance = (own_square + far_square) / D - average * average
    body = (
        part_a[...]
        + peer_a[...]
        - (average - center) * own_scale
        - (average - far_sum / features) * peer_w[0:1, :]
    )
    velocity = (
        lax.rsqrt(variance + 1e-06) * body + (own_shift + peer_w[1:2, :]) + head_bias[...]
    ).astype(jnp.bfloat16)
    to, at = iota((tokens, tokens), 0), iota((tokens, tokens), 1)
    swap = (lax.rem(to, rows_i) * cols_j + lax.div(to, rows_i) == at).astype(jnp.bfloat16)
    field = dot(swap, velocity)
    for c in noise_copies:
        c.wait()
    noises[0] = noise_own[sec]
    noise = jnp.concatenate(
        [noises[lax.rem(sec + sections - g, sections)] for g in range(sections)], axis=0
    ).astype(jnp.float32)
    std = jnp.concatenate([latent_std[...]] * 4, axis=1)
    mean_latent = jnp.concatenate([latent_mean[...]] * 4, axis=1)
    latent = (noise - step_size[0] * field) * std + mean_latent
    folded = tokens // 2
    fields[0, 0] = jnp.concatenate([latent[:folded], latent[folded:]], axis=1).astype(jnp.bfloat16)
    field_copies = spread(fields.at[0, 0], fields, field_send, field_recv)
    for c in field_copies:
        c.start()

    for c in early:
        c.wait()
    taps_in[...] = jnp.zeros_like(taps_in)
    line_size = 4 * 2 * lat
    for q in range(2):
        for e in range(3):
            col = q + e
            step_j, odd = (col + 1) // 2 - q, (col + 1) % 2
            for a in range(3):
                for b in range(3):
                    tap = 9 * a + 3 * b + e
                    for p in range(2):
                        first = step_j * 3 * line_size + a * line_size + (p + b) * 2 * lat + odd * lat
                        left = p * 2 * half
                        taps_in[q, first : first + lat, left : left + half] = in_weight[tap]
                        taps_in[q, first : first + lat, left + half : left + 2 * half] = peer_weight[tap]
    expanded[...] = jnp.zeros_like(expanded)
    wide[0] = jnp.zeros_like(wide[0])
    wide[width + 1] = jnp.zeros_like(wide[0])
    for c in field_copies:
        c.wait()

    shape = (2 * lanes, 2 * line_size)
    src, dst = iota(shape, 0), iota(shape, 1)
    same = lax.div(src, lanes) == lax.div(dst, line_size)
    src, dst = lax.rem(src, lanes), lax.rem(dst, line_size)
    place_mid = (same & (src + 2 * lat == dst)).astype(jnp.bfloat16)
    place_before = (same & (src == dst + 2 * lat) & (dst < 2 * lat)).astype(jnp.bfloat16)
    place_after = (same & (src + 6 * lat == dst) & (dst >= 6 * lat)).astype(jnp.bfloat16)
    lines_f = jnp.concatenate(
        [
            fields[slot, lax.rem(sec + sections - f, sections)]
            for slot in (1, 0)
            for f in range(frames)
        ],
        axis=0,
    ).astype(jnp.float32)
    count = 2 * frames * folded
    f_row = iota((count, 2 * lanes), 0)
    i_row = lax.rem(f_row, rows_i)
    lines_f = jnp.where((f_row >= frames * folded) | (spi > 0), lines_f, 0.0)
    before = jnp.where(i_row == 0, 0.0, pltpu.roll(lines_f, 1, 0))
    after = jnp.where(i_row == rows_i - 1, 0.0, pltpu.roll(lines_f, count - 1, 0))
    line_values = (
        dot(before.astype(jnp.bfloat16), place_before)
        + dot(lines_f.astype(jnp.bfloat16), place_mid)
        + dot(after.astype(jnp.bfloat16), place_after)
    )
    half_j = cols_j // 2
    for f in range(2 * frames):
        for side in range(2):
            expanded[1 + side * half_j : 1 + (side + 1) * half_j, f] = line_values[
                f * folded : (f + 1) * folded, side * line_size : (side + 1) * line_size
            ].reshape(half_j, rows_i, line_size)
    block = near * rows_i
    for j in range(cols_j + 2):
        for a in range(3):
            stacked[j * block : (j + 1) * block, a * line_size : (a + 1) * line_size] = (
                expanded[j, a : a + near].reshape(block, line_size).astype(jnp.bfloat16)
            )
    parts = half // channels
    tall = near * height
    for q in range(2):
        lhs = jnp.concatenate(
            [
                stacked[q * block : (q + cols_j) * block, :],
                stacked[(q + 1) * block : (q + 1 + cols_j) * block, :],
            ],
            axis=1,
        )
        for p in range(2):
            for h in range(2):
                left = (p * 2 + h) * half
                bias = in_bias[...] if h == 0 else peer_bias[...]
                up = dot(lhs, taps_in[q, :, left : left + half]) + bias
                up = up.astype(jnp.bfloat16).astype(jnp.float32)
                for j in range(cols_j):
                    for n in range(parts):
                        ups[
                            h * parts + n, pl.ds((2 * j + q) * tall + p, block, stride=2), :
                        ] = up[j * block : (j + 1) * block, n * channels : (n + 1) * channels]

    mine = lax.rem(sec + parts * core, 2 * parts)
    gain = norm_gain[pl.ds(sec, 1), :]
    h_row = lax.rem(iota((tall, channels), 0), height)
    valid = (spi > 0) | (iota((tall, channels), 0) >= 2 * height)

    def normalise(w, carry):
        at_w = pl.ds(pl.multiple_of(w * tall, tall), tall)
        squares = jnp.zeros((tall, channels), jnp.float32)
        for n in range(2 * parts):
            g = ups[n, at_w, :]
            squares = squares + g * g
        mean = jnp.sum(squares, axis=1, keepdims=True) / (2 * half)
        v = ups[mine, at_w, :] * lax.rsqrt(mean + 1e-06) * gain
        v = jnp.where(valid, v / (1.0 + jnp.exp(-v)), 0.0)
        above = jnp.where(h_row == 0, 0.0, pltpu.roll(v, 1, 0))
        below = jnp.where(h_row == height - 1, 0.0, pltpu.roll(v, tall - 1, 0))
        for b, line_v in enumerate((above, v, below)):
            wide[w + 1, :, b * channels : (b + 1) * channels] = line_v.astype(jnp.bfloat16)
        return carry

    lax.fori_loop(0, width, normalise, 0)
    loads[3].wait()

    span = frames * height

    def partial(d):
        total = jnp.zeros((columns * span, weight.shape[2]), jnp.float32)
        for a in range(3):
            for e in range(3):
                window = wide[pl.ds(d * columns + e, columns), a * height : a * height + span, :]
                taps = jnp.concatenate([weight[9 * a + 3 * b + e] for b in range(3)], axis=0)
                total = total + dot(window.reshape(columns * span, 3 * channels), taps)
        return total

    mirrored = sec >= sections // 2
    line = jnp.where(mirrored, sections - 1 - sec, sec)

    def place(n):
        return jnp.where(mirrored, sections - 1 - n, n)

    last = sections - 2
    sums = []
    for n in range(sections - 1):
        d = place(jnp.where(line == 0, sections - 1 - n, jnp.where(line <= n, n + 1, n)))
        direct = pltpu.make_async_remote_copy(
            send_buf.at[n], recv_buf.at[sec], sum_send.at[n], sum_recv.at[sec],
            device_id={"section": d},
        )
        sums.append(direct)
        if n == last:
            held[...] = partial(d)

            @pl.when(line == 1)
            def _():
                passing(send_buf.at[n], relay, sum_send.at[n], relay_sem, place(2)).wait_recv()
                held[...] += relay[...].astype(jnp.float32)

            send_buf[n] = held[...].astype(jnp.bfloat16)
            direct.start()
        elif n == 0:
            send_buf[n] = partial(d).astype(jnp.bfloat16)

            @pl.when(line == 0)
            def _():
                passing(send_buf.at[n], relay, sum_send.at[n], relay_sem, place(1)).start()

            @pl.when(line != 0)
            def _():
                direct.start()
        else:
            send_buf[n] = partial(d).astype(jnp.bfloat16)
            direct.start()
    total = partial(sec) + conv_bias[...]
    total = total.reshape(columns, span, half)
    own_w = []
    for w in range(columns):
        first = pl.multiple_of((sec * columns + w) * tall + 2 * height, height)
        own_w.append(
            jnp.concatenate([ups[n, pl.ds(first, span), :] for n in range(parts)], axis=1)
        )
    total = total + jnp.stack(own_w)
    for c in sums:
        c.wait_send()
    held[...] = total.reshape(held.shape)
    for g in range(sections):
        gap = jnp.abs(sec - g)

        @pl.when((gap > 0) & (gap < sections - 1))
        def _():
            passing(send_buf.at[0], recv_buf.at[g], sum_send.at[0], sum_recv.at[g], g).wait_recv()
            held[...] += recv_buf[g].astype(jnp.float32)

    total = held[...].reshape(columns, span, half)
    for w in range(columns):
        for n in range(parts):
            final[n, pl.ds(w, span, stride=columns), :] = total[
                w, :, n * channels : (n + 1) * channels
            ]
    for n in range(parts):
        out[:, n * channels : (n + 1) * channels] = final[n].astype(out.dtype)


def fused_shards(sizes, *arrays):
    (
        hidden, modulation, time_embed, head_weight, head_bias, noisy, step_size, latent_mean,
        latent_std, in_weight, in_bias, norm_gain, conv_weight, conv_bias,
    ) = arrays
    sections, clips_sp, frames, height, columns, lat, channels = sizes
    rows_i, cols_j, half = height // 2, columns * sections // 2, in_weight.shape[2]
    width, near, tokens, lanes = columns * sections, frames + 2, hidden.shape[0], 4 * lat
    line_size = 8 * lat
    f32, bf16 = jnp.float32, jnp.bfloat16
    vmem, dma = pltpu.VMEM, pltpu.SemaphoreType.DMA
    in_vmem = pl.BlockSpec(memory_space=pltpu.VMEM)
    rows = columns * frames * height
    out = pl.pallas_call(
        functools.partial(block_kernel, sizes),
        out_shape=jax.ShapeDtypeStruct((rows, half), bf16),
        in_specs=[in_vmem] * 4
        + [pl.BlockSpec(memory_space=pltpu.SMEM)]
        + [in_vmem] * 5
        + [pl.BlockSpec(memory_space=pl.ANY)] * 4,
        out_specs=in_vmem,
        scratch_shapes=[
            vmem(hidden.shape, bf16),
            vmem(head_weight.shape[::-1], bf16),
            vmem(in_weight.shape, bf16),
            vmem((tokens, lanes), f32),
            vmem((tokens, 128), f32),
            vmem((8, lanes), f32),
            vmem((tokens, lanes), f32),
            vmem((tokens, 128), f32),
            vmem((8, lanes), f32),
            vmem(in_weight.shape, bf16),
            vmem((1, half), f32),
            vmem((2, sections, tokens // 2, 2 * lanes), bf16),
            vmem((sections, tokens // sections, lanes), bf16),
            vmem((frames, tokens // sections, lanes), bf16),
            vmem((cols_j + 2, 2 * frames, rows_i, line_size), f32),
            vmem(((cols_j + 2) * near * rows_i, 3 * line_size), bf16),
            vmem((2, 6 * line_size, 4 * half), bf16),
            vmem((2 * half // channels, width * near * height, channels), f32),
            vmem((width + 2, near * height, 3 * channels), bf16),
            vmem(conv_weight.shape, bf16),
            vmem((sections, rows, half), bf16),
            vmem((sections, rows, half), bf16),
            vmem((rows, half), bf16),
            vmem((rows, half), f32),
            vmem((half // channels, rows, channels), f32),
            dma((4,)),
            dma,
            dma((5,)),
            dma((5,)),
            dma((sections,)),
            dma((sections,)),
            dma((2, sections)),
            dma((2, sections)),
            dma((sections,)),
            dma((sections,)),
        ],
        compiler_params=pltpu.CompilerParams(collective_id=0, has_side_effects=True),
    )(
        modulation, time_embed[None], head_bias[None], noisy.reshape(-1, lat), step_size,
        latent_std[None], latent_mean[None], in_bias[None], norm_gain.reshape(-1, channels),
        conv_bias[None], hidden, head_weight.T, in_weight, conv_weight,
    )
    return out.reshape(frames, height, columns, half)


def dispatch(*arrays):
    hidden, noisy, in_weight, conv_weight = arrays[0], arrays[5], arrays[9], arrays[12]
    frames, height, columns, lat = noisy.shape
    sections, cores, clips_sp = (lax.axis_size(axis) for axis in ("section", "tp", "sp"))
    channels, half = conv_weight.shape[1:]
    whole_frame = hidden.shape[0] == height // 2 * (columns * sections // 2)
    if (
        whole_frame
        and cores == 2
        and clips_sp > 1
        and frames == sections
        and sections > 3
        and channels % 128 == 0
        and half % channels == 0
        and lat == 16
        and height == 16
    ):
        sizes = (sections, clips_sp, frames, height, columns, lat, channels)
        return fused_shards(sizes, *arrays)
    return shards(*arrays)


def solution(mesh):
    placed = (
        P(("groups", "sp", "section"), "tp"),
        P(None, "tp"),
        P(("groups", "tp")),
        P("tp", None),
        P(),
        P(("groups", "sp"), None, "section", None),
        P("groups"),
        P(),
        P(),
        P(None, None, "tp"),
        P("tp"),
        P(),
        P(None, "section", "tp"),
        P("tp"),
    )
    return jax.shard_map(
        dispatch,
        mesh=mesh,
        in_specs=placed,
        out_specs=P(("groups", "sp"), None, "section", "tp"),
        check_vma=False,
    )
```

```python
import functools

import jax
import jax.numpy as jnp
from jax import lax
from jax.experimental import pallas as pl
from jax.experimental.pallas import tpu as pltpu
from jax.sharding import PartitionSpec as P

D = 6144


def padded_2(value, sides, width):
    for axis, dim in sides:
        count, length = (lax.axis_size(axis), value.shape[dim])
        up = [(i, (i + 1) % count) for i in range(count - 1)]
        down = [(j, i) for i, j in up]
        last = lax.slice_in_dim(value, length - width, length, axis=dim)
        leading = lax.slice_in_dim(value, 0, width, axis=dim)
        before = lax.ppermute(last, axis, up)
        after = lax.ppermute(leading, axis, down)
        value = jnp.concatenate([before, value, after], axis=dim)
    return value


def passed_along(value, axis, by):
    count = lax.axis_size(axis)
    pairs = [(i, i + by) for i in range(count) if 0 <= i + by < count]
    return lax.ppermute(value, axis, pairs)


def conv_taps(padded, weight, frames, height, columns):
    channels = padded.shape[3]
    result = jnp.zeros((frames * height * columns, weight.shape[2]), jnp.float32)
    for offset_time in range(3):
        for offset_row in range(3):
            slab = padded[offset_time : offset_time + frames, offset_row : offset_row + height]
            window = jnp.concatenate(
                [slab[:, :, 0:columns], slab[:, :, 1 : columns + 1], slab[:, :, 2 : columns + 2]],
                axis=3,
            )
            first = 9 * offset_time + 3 * offset_row
            taps = weight[first : first + 3].reshape(3 * channels, weight.shape[2])
            result = result + jnp.dot(
                window.reshape(-1, 3 * channels), taps, preferred_element_type=jnp.float32
            )
    return result


def activate(source, gain_vector):
    values = source.astype(jnp.float32)
    squares = jnp.mean(values * values, axis=-1, keepdims=True)
    return jax.nn.silu(values * lax.rsqrt(squares + 1e-06) * gain_vector).astype(jnp.bfloat16)


def pad_rows(source):
    return jnp.pad(source, ((0, 0), (1, 1), (0, 0), (0, 0)))


def shards(
    hidden,
    modulation,
    time_embed,
    head_weight,
    head_bias,
    noisy,
    step_size,
    latent_mean,
    latent_std,
    in_weight,
    in_bias,
    norm_gain,
    conv_weight,
    conv_bias,
):
    frames, height, columns, lat_channels = noisy.shape
    sections = lax.axis_size("section")
    half_channels = in_weight.shape[2]
    values = hidden.astype(jnp.float32)
    row_sums, square_sums = lax.psum(
        (jnp.sum(values, axis=1), jnp.sum(values * values, axis=1)), "tp"
    )
    average = row_sums / D
    variance = square_sums / D - average * average
    shift_term = modulation[0] + time_embed
    scale_term = modulation[1] + time_embed
    modulated = (
        (values - average[:, None]) * lax.rsqrt(variance[:, None] + 1e-06) * (1.0 + scale_term)
        + shift_term
    ).astype(jnp.bfloat16)
    partial_sum = jnp.dot(modulated, head_weight, preferred_element_type=jnp.float32)
    velocity = (lax.psum(partial_sum, "tp") + head_bias).astype(jnp.bfloat16)
    band_rows = velocity.shape[0] * 2 // (columns * sections)
    outgoing = velocity.reshape(band_rows, sections, -1)
    arrived = lax.all_to_all(outgoing, "section", split_axis=1, concat_axis=0, tiled=True)
    latent_field = arrived.reshape(frames, height // 2, columns // 2, 2, 2, lat_channels)
    latent_field = jnp.transpose(latent_field, (0, 1, 3, 2, 4, 5)).reshape(
        frames, height, columns, lat_channels
    )
    latent = (
        (noisy.astype(jnp.float32) - step_size[0] * latent_field.astype(jnp.float32)) * latent_std
        + latent_mean
    ).astype(jnp.bfloat16)
    latent_wide = padded_2(latent, (("section", 2),), 2)
    earlier = passed_along(latent_wide, "sp", 1)
    stacked = pad_rows(jnp.concatenate([earlier, latent_wide], axis=0))
    extended = (conv_taps(stacked, in_weight, frames + 2, height, columns + 2) + in_bias).astype(
        jnp.bfloat16
    )
    extended = extended.reshape(frames + 2, height, columns + 2, half_channels)
    upblock_half = extended[2:, :, 1 : columns + 1]
    extended_full = lax.all_gather(extended, "tp", axis=3, tiled=True)
    normed = activate(extended_full, norm_gain)
    frame_index = lax.axis_index("sp") * frames - 2 + jnp.arange(frames + 2, dtype=jnp.int32)
    column_index = (
        lax.axis_index("section") * columns - 1 + jnp.arange(columns + 2, dtype=jnp.int32)
    )
    inside_cols = (column_index >= 0) & (column_index < columns * sections)
    inside = (frame_index >= 0)[:, None, None, None] & inside_cols[None, None, :, None]
    conv_input = pad_rows(jnp.where(inside, normed, jnp.zeros_like(normed)))
    full_weight = lax.all_gather(conv_weight, "section", axis=1, tiled=True)
    mixed = conv_taps(conv_input, full_weight, frames, height, columns)
    decoded = (
        upblock_half.astype(jnp.float32).reshape(-1, half_channels) + mixed + conv_bias
    ).astype(jnp.bfloat16)
    return decoded.reshape(frames, height, columns, half_channels)


def iota(shape, dim):
    return lax.broadcasted_iota(jnp.int32, shape, dim)


def dot(left, right):
    return jnp.dot(left, right, preferred_element_type=jnp.float32)


def dot_rows(left, right):
    return lax.dot_general(
        left, right, (((1,), (1,)), ((), ())), preferred_element_type=jnp.float32
    )


def pieces(value):
    high = value.astype(jnp.bfloat16)
    rest = value - high.astype(jnp.float32)
    middle = rest.astype(jnp.bfloat16)
    low = (rest - middle.astype(jnp.float32)).astype(jnp.bfloat16)
    return high.astype(jnp.float32), middle.astype(jnp.float32), low.astype(jnp.float32)


def block_kernel(
    sizes,
    modulation,
    time_embed,
    head_bias,
    noisy,
    step_size,
    latent_std,
    latent_mean,
    in_bias,
    norm_gain,
    conv_bias,
    hidden_far,
    head_far,
    in_far,
    conv_far,
    out,
    hidden,
    head_weight,
    in_weight,
    part_a,
    part_s,
    part_w,
    peer_a,
    peer_s,
    peer_w,
    peer_weight,
    peer_bias,
    fields,
    noises,
    noise_own,
    expanded,
    stacked,
    taps_in,
    ups,
    wide,
    weight,
    send_buf,
    recv_buf,
    final,
    load_sems,
    pair_send,
    pair_recv,
    noise_send,
    noise_recv,
    field_send,
    field_recv,
    sum_send,
    sum_recv,
):
    sections, clips_sp, frames, height, columns, lat, channels = sizes
    rows_i, cols_j = height // 2, columns * sections // 2
    width = columns * sections
    tokens = rows_i * cols_j
    near = frames + 2
    half = in_weight.shape[2]
    sec, core, spi = lax.axis_index("section"), lax.axis_index("tp"), lax.axis_index("sp")
    nxt, prv = lax.rem(spi + 1, clips_sp), lax.rem(spi + clips_sp - 1, clips_sp)
    peer = {"tp": 1 - core}

    loads = [
        pltpu.make_async_copy(source, target, load_sems.at[n])
        for n, (source, target) in enumerate(
            ((hidden_far, hidden), (head_far, head_weight), (in_far, in_weight), (conv_far, weight))
        )
    ]
    for c in loads:
        c.start()
    barrier = pltpu.get_barrier_semaphore()
    pl.semaphore_signal(barrier, inc=1, device_id=peer)
    for k in range(1, sections):
        pl.semaphore_signal(barrier, inc=1, device_id={"section": lax.rem(sec + k, sections)})
    for k in range(sections):
        pl.semaphore_signal(
            barrier, inc=1, device_id={"section": lax.rem(sec + k, sections), "sp": prv}
        )

    def pair_copy(n, source, target):
        return pltpu.make_async_remote_copy(
            source, target, pair_send.at[n], pair_recv.at[n], device_id=peer
        )

    def spread(source, target, send, recv):
        made = []
        for k in range(1, sections):
            made.append(
                pltpu.make_async_remote_copy(
                    source, target.at[0, k], send.at[0, k], recv.at[0, k],
                    device_id={"section": lax.rem(sec + k, sections)},
                )
            )
        for k in range(sections):
            made.append(
                pltpu.make_async_remote_copy(
                    source, target.at[1, k], send.at[1, k], recv.at[1, k],
                    device_id={"section": lax.rem(sec + k, sections), "sp": nxt},
                )
            )
        return made

    lanes = 4 * lat
    tile = rows_i * columns // 2
    share = frames * tile
    to, at = iota((4 * share, 4 * share), 0), iota((4 * share, 4 * share), 1)
    cell, token = lax.div(to, share), lax.rem(to, share)
    line_f = lax.div(token, tile)
    jl, line_i = lax.div(lax.rem(token, tile), rows_i), line_f * rows_i + lax.rem(token, rows_i)
    home = (2 * line_i + lax.div(cell, 2)) * columns + 2 * jl + lax.rem(cell, 2)
    moved = dot((home == at).astype(jnp.bfloat16), noisy[...]).astype(jnp.bfloat16)
    src, dst = iota((lat, lanes), 0), iota((lat, lanes), 1)
    own_noise = jnp.zeros((share, lanes), jnp.float32)
    for n in range(4):
        own_noise = own_noise + dot(
            moved[n * share : (n + 1) * share], (src + n * lat == dst).astype(jnp.bfloat16)
        )
    noise_own[...] = own_noise.astype(jnp.bfloat16).reshape(noise_own.shape)

    features = hidden.shape[1]
    scale = 1.0 + (modulation[1:2, :] + time_embed[...])
    shift = modulation[0:1, :] + time_embed[...]
    loads[0].wait()
    values = hidden[...].astype(jnp.float32)
    own_sum = jnp.sum(values, axis=1, keepdims=True)
    own_square = jnp.sum(values * values, axis=1, keepdims=True)
    center = own_sum / features
    centred = ((values - center) * scale).astype(jnp.bfloat16)
    loads[1].wait()
    part_a[...] = dot_rows(centred, head_weight[...])
    part_s[...] = jnp.where(iota(part_s.shape, 1) < part_s.shape[1] // 2, own_sum, own_square)
    row = iota((8, features), 0)
    lines = jnp.zeros((8, features), jnp.float32)
    for n, piece in enumerate(pieces(scale) + pieces(shift)):
        lines = jnp.where(row == n, piece, lines)
    made = dot_rows(lines.astype(jnp.bfloat16), head_weight[...])
    line = iota(made.shape, 0)
    own_scale = jnp.sum(jnp.where(line < 3, made, 0.0), axis=0, keepdims=True)
    own_shift = jnp.sum(jnp.where(line >= 3, made, 0.0), axis=0, keepdims=True)
    part_w[...] = jnp.where(line == 0, own_scale, own_shift)
    pair = [
        pair_copy(2, part_a, peer_a), pair_copy(3, part_s, peer_s), pair_copy(4, part_w, peer_w)
    ]
    loads[2].wait()
    early = [pair_copy(0, in_weight, peer_weight), pair_copy(1, in_bias, peer_bias)]
    noise_copies = []
    for k in range(1, sections):
        d = lax.rem(sec + k, sections)
        noise_copies.append(
            pltpu.make_async_remote_copy(
                noise_own.at[d], noises.at[k], noise_send.at[k], noise_recv.at[k],
                device_id={"section": d},
            )
        )
    pl.semaphore_wait(barrier, 2 * sections)
    for c in pair + noise_copies + early:
        c.start()
    for c in pair:
        c.wait()
    far_sum = peer_s[:, 0:1]
    far_square = peer_s[:, part_s.shape[1] // 2 : part_s.shape[1] // 2 + 1]
    average = (own_sum + far_sum) / D
    variance = (own_square + far_square) / D - average * average
    body = (
        part_a[...]
        + peer_a[...]
        - (average - center) * own_scale
        - (average - far_sum / features) * peer_w[0:1, :]
    )
    velocity = (
        lax.rsqrt(variance + 1e-06) * body + (own_shift + peer_w[1:2, :]) + head_bias[...]
    ).astype(jnp.bfloat16)
    to, at = iota((tokens, tokens), 0), iota((tokens, tokens), 1)
    swap = (lax.rem(to, rows_i) * cols_j + lax.div(to, rows_i) == at).astype(jnp.bfloat16)
    field = dot(swap, velocity)
    for c in noise_copies:
        c.wait()
    noises[0] = noise_own[sec]
    noise = jnp.concatenate(
        [noises[lax.rem(sec + sections - g, sections)] for g in range(sections)], axis=0
    ).astype(jnp.float32)
    std = jnp.concatenate([latent_std[...]] * 4, axis=1)
    mean_latent = jnp.concatenate([latent_mean[...]] * 4, axis=1)
    latent = (noise - step_size[0] * field) * std + mean_latent
    folded = tokens // 2
    fields[0, 0] = jnp.concatenate([latent[:folded], latent[folded:]], axis=1).astype(jnp.bfloat16)
    field_copies = spread(fields.at[0, 0], fields, field_send, field_recv)
    for c in field_copies:
        c.start()

    for c in early:
        c.wait()
    taps_in[...] = jnp.zeros_like(taps_in)
    line_size = 4 * 2 * lat
    for q in range(2):
        for e in range(3):
            col = q + e
            step_j, odd = (col + 1) // 2 - q, (col + 1) % 2
            for a in range(3):
                for b in range(3):
                    tap = 9 * a + 3 * b + e
                    for p in range(2):
                        first = step_j * 3 * line_size + a * line_size + (p + b) * 2 * lat + odd * lat
                        left = p * 2 * half
                        taps_in[q, first : first + lat, left : left + half] = in_weight[tap]
                        taps_in[q, first : first + lat, left + half : left + 2 * half] = peer_weight[tap]
    expanded[...] = jnp.zeros_like(expanded)
    wide[0] = jnp.zeros_like(wide[0])
    wide[width + 1] = jnp.zeros_like(wide[0])
    for c in field_copies:
        c.wait()

    shape = (2 * lanes, 2 * line_size)
    src, dst = iota(shape, 0), iota(shape, 1)
    same = lax.div(src, lanes) == lax.div(dst, line_size)
    src, dst = lax.rem(src, lanes), lax.rem(dst, line_size)
    place_mid = (same & (src + 2 * lat == dst)).astype(jnp.bfloat16)
    place_before = (same & (src == dst + 2 * lat) & (dst < 2 * lat)).astype(jnp.bfloat16)
    place_after = (same & (src + 6 * lat == dst) & (dst >= 6 * lat)).astype(jnp.bfloat16)
    lines_f = jnp.concatenate(
        [
            fields[slot, lax.rem(sec + sections - f, sections)]
            for slot in (1, 0)
            for f in range(frames)
        ],
        axis=0,
    ).astype(jnp.float32)
    count = 2 * frames * folded
    f_row = iota((count, 2 * lanes), 0)
    i_row = lax.rem(f_row, rows_i)
    lines_f = jnp.where((f_row >= frames * folded) | (spi > 0), lines_f, 0.0)
    before = jnp.where(i_row == 0, 0.0, pltpu.roll(lines_f, 1, 0))
    after = jnp.where(i_row == rows_i - 1, 0.0, pltpu.roll(lines_f, count - 1, 0))
    line_values = (
        dot(before.astype(jnp.bfloat16), place_before)
        + dot(lines_f.astype(jnp.bfloat16), place_mid)
        + dot(after.astype(jnp.bfloat16), place_after)
    )
    half_j = cols_j // 2
    for f in range(2 * frames):
        for side in range(2):
            expanded[1 + side * half_j : 1 + (side + 1) * half_j, f] = line_values[
                f * folded : (f + 1) * folded, side * line_size : (side + 1) * line_size
            ].reshape(half_j, rows_i, line_size)
    block = near * rows_i
    for j in range(cols_j + 2):
        for a in range(3):
            stacked[j * block : (j + 1) * block, a * line_size : (a + 1) * line_size] = (
                expanded[j, a : a + near].reshape(block, line_size).astype(jnp.bfloat16)
            )
    parts = half // channels
    tall = near * height
    for q in range(2):
        lhs = jnp.concatenate(
            [
                stacked[q * block : (q + cols_j) * block, :],
                stacked[(q + 1) * block : (q + 1 + cols_j) * block, :],
            ],
            axis=1,
        )
        for p in range(2):
            for h in range(2):
                left = (p * 2 + h) * half
                bias = in_bias[...] if h == 0 else peer_bias[...]
                up = dot(lhs, taps_in[q, :, left : left + half]) + bias
                up = up.astype(jnp.bfloat16).astype(jnp.float32)
                for j in range(cols_j):
                    for n in range(parts):
                        ups[
                            h * parts + n, pl.ds((2 * j + q) * tall + p, block, stride=2), :
                        ] = up[j * block : (j + 1) * block, n * channels : (n + 1) * channels]

    mine = lax.rem(sec + parts * core, 2 * parts)
    gain = norm_gain[pl.ds(sec, 1), :]
    h_row = lax.rem(iota((tall, channels), 0), height)
    valid = (spi > 0) | (iota((tall, channels), 0) >= 2 * height)

    def normalise(w, carry):
        at_w = pl.ds(pl.multiple_of(w * tall, tall), tall)
        squares = jnp.zeros((tall, channels), jnp.float32)
        for n in range(2 * parts):
            g = ups[n, at_w, :]
            squares = squares + g * g
        mean = jnp.sum(squares, axis=1, keepdims=True) / (2 * half)
        v = ups[mine, at_w, :] * lax.rsqrt(mean + 1e-06) * gain
        v = jnp.where(valid, v / (1.0 + jnp.exp(-v)), 0.0)
        above = jnp.where(h_row == 0, 0.0, pltpu.roll(v, 1, 0))
        below = jnp.where(h_row == height - 1, 0.0, pltpu.roll(v, tall - 1, 0))
        for b, line_v in enumerate((above, v, below)):
            wide[w + 1, :, b * channels : (b + 1) * channels] = line_v.astype(jnp.bfloat16)
        return carry

    lax.fori_loop(0, width, normalise, 0)
    loads[3].wait()

    span = frames * height

    def partial(d):
        total = jnp.zeros((columns * span, weight.shape[2]), jnp.float32)
        for a in range(3):
            for e in range(3):
                window = wide[pl.ds(d * columns + e, columns), a * height : a * height + span, :]
                taps = jnp.concatenate([weight[9 * a + 3 * b + e] for b in range(3)], axis=0)
                total = total + dot(window.reshape(columns * span, 3 * channels), taps)
        return total

    sums = []
    for k in [*range(sections // 2, sections), *range(1, sections // 2)]:
        d = lax.rem(sec + k, sections)
        send_buf[k] = partial(d).astype(jnp.bfloat16)
        c = pltpu.make_async_remote_copy(
            send_buf.at[k], recv_buf.at[k], sum_send.at[k], sum_recv.at[k],
            device_id={"section": d},
        )
        c.start()
        sums.append(c)
    total = partial(sec) + conv_bias[...]
    total = total.reshape(columns, span, half)
    own_w = []
    for w in range(columns):
        first = pl.multiple_of((sec * columns + w) * tall + 2 * height, height)
        own_w.append(
            jnp.concatenate([ups[n, pl.ds(first, span), :] for n in range(parts)], axis=1)
        )
    total = total + jnp.stack(own_w)
    for c in sums:
        c.wait()
    for k in range(1, sections):
        total = total + recv_buf[k].astype(jnp.float32).reshape(columns, span, half)
    for w in range(columns):
        for n in range(parts):
            final[n, pl.ds(w, span, stride=columns), :] = total[
                w, :, n * channels : (n + 1) * channels
            ]
    for n in range(parts):
        out[:, n * channels : (n + 1) * channels] = final[n].astype(out.dtype)


def fused_shards(sizes, *arrays):
    (
        hidden, modulation, time_embed, head_weight, head_bias, noisy, step_size, latent_mean,
        latent_std, in_weight, in_bias, norm_gain, conv_weight, conv_bias,
    ) = arrays
    sections, clips_sp, frames, height, columns, lat, channels = sizes
    rows_i, cols_j, half = height // 2, columns * sections // 2, in_weight.shape[2]
    width, near, tokens, lanes = columns * sections, frames + 2, hidden.shape[0], 4 * lat
    line_size = 8 * lat
    f32, bf16 = jnp.float32, jnp.bfloat16
    vmem, dma = pltpu.VMEM, pltpu.SemaphoreType.DMA
    in_vmem = pl.BlockSpec(memory_space=pltpu.VMEM)
    rows = columns * frames * height
    out = pl.pallas_call(
        functools.partial(block_kernel, sizes),
        out_shape=jax.ShapeDtypeStruct((rows, half), bf16),
        in_specs=[in_vmem] * 4
        + [pl.BlockSpec(memory_space=pltpu.SMEM)]
        + [in_vmem] * 5
        + [pl.BlockSpec(memory_space=pl.ANY)] * 4,
        out_specs=in_vmem,
        scratch_shapes=[
            vmem(hidden.shape, bf16),
            vmem(head_weight.shape[::-1], bf16),
            vmem(in_weight.shape, bf16),
            vmem((tokens, lanes), f32),
            vmem((tokens, 128), f32),
            vmem((8, lanes), f32),
            vmem((tokens, lanes), f32),
            vmem((tokens, 128), f32),
            vmem((8, lanes), f32),
            vmem(in_weight.shape, bf16),
            vmem((1, half), f32),
            vmem((2, sections, tokens // 2, 2 * lanes), bf16),
            vmem((sections, tokens // sections, lanes), bf16),
            vmem((frames, tokens // sections, lanes), bf16),
            vmem((cols_j + 2, 2 * frames, rows_i, line_size), f32),
            vmem(((cols_j + 2) * near * rows_i, 3 * line_size), bf16),
            vmem((2, 6 * line_size, 4 * half), bf16),
            vmem((2 * half // channels, width * near * height, channels), f32),
            vmem((width + 2, near * height, 3 * channels), bf16),
            vmem(conv_weight.shape, bf16),
            vmem((sections, rows, half), bf16),
            vmem((sections, rows, half), bf16),
            vmem((half // channels, rows, channels), f32),
            dma((4,)),
            dma((5,)),
            dma((5,)),
            dma((sections,)),
            dma((sections,)),
            dma((2, sections)),
            dma((2, sections)),
            dma((sections,)),
            dma((sections,)),
        ],
        compiler_params=pltpu.CompilerParams(collective_id=0, has_side_effects=True),
    )(
        modulation, time_embed[None], head_bias[None], noisy.reshape(-1, lat), step_size,
        latent_std[None], latent_mean[None], in_bias[None], norm_gain.reshape(-1, channels),
        conv_bias[None], hidden, head_weight.T, in_weight, conv_weight,
    )
    return out.reshape(frames, height, columns, half)


def dispatch(*arrays):
    hidden, noisy, in_weight, conv_weight = arrays[0], arrays[5], arrays[9], arrays[12]
    frames, height, columns, lat = noisy.shape
    sections, cores, clips_sp = (lax.axis_size(axis) for axis in ("section", "tp", "sp"))
    channels, half = conv_weight.shape[1:]
    whole_frame = hidden.shape[0] == height // 2 * (columns * sections // 2)
    if (
        whole_frame
        and cores == 2
        and clips_sp > 1
        and frames == sections
        and channels % 128 == 0
        and half % channels == 0
        and lat == 16
        and height == 16
    ):
        sizes = (sections, clips_sp, frames, height, columns, lat, channels)
        return fused_shards(sizes, *arrays)
    return shards(*arrays)


def solution(mesh):
    placed = (
        P(("groups", "sp", "section"), "tp"),
        P(None, "tp"),
        P(("groups", "tp")),
        P("tp", None),
        P(),
        P(("groups", "sp"), None, "section", None),
        P("groups"),
        P(),
        P(),
        P(None, None, "tp"),
        P("tp"),
        P(),
        P(None, "section", "tp"),
        P("tp"),
    )
    return jax.shard_map(
        dispatch,
        mesh=mesh,
        in_specs=placed,
        out_specs=P(("groups", "sp"), None, "section", "tp"),
        check_vma=False,
    )
```
